512 devices in a mesh: frame: 32 (over y_lo, z, core), space: 16 (over x, y_hi).
Axes of the slice: x: 4, y: 8 (y_hi: 4, y_lo: 2; y = y_hi * 2 + y_lo), z: 8, core: 2. Of those that a mesh axis runs over, the one named last changes fastest.
Arguments:
- spatial_query: bfloat16 [32, 1024, 1152], P('frame', 'space'), may hold values from -24 to 24
- spatial_key: bfloat16 [32, 1024, 1152], P('frame', 'space'), may hold values from -24 to 24
- spatial_value: bfloat16 [32, 1024, 1152], P('frame', 'space'), may hold values from -6 to 6
- latents: bfloat16 [32, 1024, 1152], P('frame', 'space'), may hold values from -6 to 6
- proj_weight: bfloat16 [1152, 1152], P('frame'), may hold values from -0.1875 to 0.1875
- proj_bias: float32 [1152], replicated, may hold values from -3 to 3
- residual_gate: float32 [1152], replicated, may hold values from 0.5 to 1.5
- temporal_shift: float32 [1152], replicated, may hold values from -3 to 3
- temporal_scale: float32 [1152], replicated, may hold values from -0.5 to 0.5
- temporal_weight: bfloat16 [1152, 3456], P('frame'), may hold values from -0.75 to 0.75
- clip_lengths: int32 [16], replicated, may hold values from 1 to 4, 32 in all
Outputs:
- hidden: float32 [32, 1024, 1152], P('frame', 'space')
- temporal_out: float32 [32, 1024, 1152], P('frame', 'space')
The draws below stay inside these ranges and needn't reach their ends.
Inputs may be any that keep to these rules, and one draw needn't show every extreme that they name: `clip_lengths`: 16 clips fill the 32 frames in order; one clip has exactly 4 frames.
All inputs are finite; a program needn't handle non-finite values.
Results may differ from the reference program's by a relative error of at most 0.012.
Values may be sent and summed in bfloat16 or wider, within the bound.
A program may use at most 64 MiB of HBM per device.

```python
import math
import jax
import jax.numpy as jnp
import numpy as np
from jax import lax

D = 1152
HEADS = 16
FRAMES = 32
PATCHES = 1024
CLIPS = 16
MOST = 4


def boosted_heads(key):
    base = jnp.clip(2.0 * jax.random.normal(key, (FRAMES, PATCHES, D), jnp.float32), -8.0, 8.0)
    return base


def draw_spatial_query(key, part):
    return boosted_heads(jax.random.fold_in(key, 11)).astype(jnp.bfloat16)


def draw_spatial_key(key, part):
    return boosted_heads(jax.random.fold_in(key, 12)).astype(jnp.bfloat16)


def draw_temporal_weight(key, part):
    base = jnp.clip(jax.random.normal(jax.random.fold_in(key, 13), (D, 3 * D), jnp.float32), -4.0, 4.0)
    return jnp.clip(base * (1.0 / math.sqrt(D)), -0.75, 0.75).astype(jnp.bfloat16)


def block_scale(rng, extent, cuts, smallest, largest):
    def one(dim, parts):
        steps = jax.random.uniform(jax.random.fold_in(jax.random.fold_in(rng, 6), dim), (parts,), jnp.float32, smallest / len(cuts), largest / len(cuts))
        return jnp.repeat(jnp.exp(steps), extent[dim] // parts).reshape((-1,) + (1,) * (len(extent) - dim - 1))

    level = one(*cuts[0])
    for cut in cuts[1:]:
        level = level * one(*cut)
    return level


def profile(amount, total, reach, lean):
    loads = [(1 << 20) // math.isqrt(standing ** lean) + 1 for standing in range(2, amount + 1)]
    rest, counts = total - reach - (amount - 1), [1] * (amount - 1)
    while rest > 0:
        free = [i for i in range(amount - 1) if counts[i] < reach]
        mass, left = sum([loads[i] for i in free]), rest
        for i in free:
            more = min(reach - counts[i], max(1, left * loads[i] // mass), rest)
            counts[i] = counts[i] + more
            rest = rest - more
    return np.array([reach] + counts)


def uneven(rng, count, total, reach, skew):
    if count == 2:
        one = jax.random.randint(rng, (), max(1, total - reach), min(reach, total - 1) + 1)
        return jnp.stack([one, total - one])
    tallies = jnp.asarray(profile(count, total, reach, skew), jnp.int32)
    pairs = (count - 1) // 2
    giver, sink = tallies[1:1 + 2 * pairs:2], tallies[2:2 + 2 * pairs:2]
    slack = jnp.minimum(giver - 1, reach - sink)
    passed = jax.random.randint(jax.random.fold_in(rng, 1), (pairs,), 0, 1 << 20) % (slack + 1)
    tallies = tallies.at[1:1 + 2 * pairs:2].set(giver - passed).at[2:2 + 2 * pairs:2].set(sink + passed)
    return tallies[jax.random.permutation(jax.random.fold_in(rng, 2), count)]


def bell_draw(own_key, dims, deviation, limit, shards=(), kind=jnp.bfloat16):
    values = jax.random.normal(own_key, dims, jnp.float32) * deviation
    if len(shards) > 0:
        values = block_scale(own_key, dims, shards, -0.22, 0.18) * values
    return jnp.clip(values, min=-limit, max=limit).astype(kind)


def setup_inputs(seed: int = 0) -> dict:
    splits = jax.random.split(jax.random.key(seed), 12)
    return {
        "spatial_query": draw_spatial_query(jax.random.fold_in(splits[11], 71), 0),
        "spatial_key": draw_spatial_key(jax.random.fold_in(splits[11], 71), 0),
        "spatial_value": bell_draw(splits[2], (FRAMES, PATCHES, D), 1.0, 6.0, ((0, 32), (1, 16))),
        "latents": bell_draw(splits[3], (FRAMES, PATCHES, D), 1.0, 6.0, ((0, 32), (1, 16))),
        "proj_weight": bell_draw(splits[4], (D, D), D ** -0.5, 0.1875, ((0, 32),)),
        "proj_bias": bell_draw(splits[5], (D,), 0.5, 3.0, (), jnp.float32),
        "residual_gate": jnp.clip(jax.random.uniform(splits[6], (D,), jnp.float32, 0.5, 1.5), 0.5, 1.5),
        "temporal_shift": bell_draw(splits[7], (D,), 0.5, 3.0, (), jnp.float32),
        "temporal_scale": jnp.clip(jax.random.uniform(splits[8], (D,), jnp.float32, -0.5, 0.5), -0.5, 0.5),
        "temporal_weight": draw_temporal_weight(jax.random.fold_in(splits[11], 71), 0),
        "clip_lengths": uneven(splits[10], CLIPS, FRAMES, MOST, 2).astype(jnp.int32),
    }


def attend(query, keys, values, allowed):
    scale = 1.0 / math.sqrt(query.shape[-1])
    scores = jnp.einsum('qhd,khd->hqk', query.astype(jnp.float32), keys.astype(jnp.float32)) * scale
    if allowed is not None:
        scores = jnp.where(allowed[None, :, :], scores, -1e+30)
    top = lax.optimization_barrier(jnp.max(scores, axis=-1, keepdims=True))
    probs = jnp.exp(scores - top)
    total = lax.optimization_barrier(jnp.sum(probs, axis=-1))
    weights = lax.optimization_barrier(probs.astype(jnp.bfloat16))
    mixed = jnp.einsum('hqk,khd->qhd', weights.astype(jnp.float32), values.astype(jnp.float32))
    return mixed / jnp.transpose(total)[:, :, None]

def reference(spatial_query, spatial_key, spatial_value, latents, proj_weight, proj_bias, residual_gate, temporal_shift, temporal_scale, temporal_weight, clip_lengths):
    head_dim = D // HEADS

    def one_frame(frame):
        fq, fk, fv = frame
        split = (PATCHES, HEADS, head_dim)
        return attend(fq.reshape(split), fk.reshape(split), fv.reshape(split), None).reshape(PATCHES, D).astype(jnp.bfloat16)
    attended = lax.map(one_frame, (spatial_query, spatial_key, spatial_value))
    flat = attended.reshape(FRAMES * PATCHES, D)
    projected = jnp.dot(flat, proj_weight, preferred_element_type=jnp.float32)
    hidden = latents.reshape(FRAMES * PATCHES, D).astype(jnp.float32) + residual_gate * (projected + proj_bias)
    mean = lax.optimization_barrier(jnp.mean(hidden, axis=-1, keepdims=True))
    centred = hidden - mean
    variance = lax.optimization_barrier(jnp.mean(centred * centred, axis=-1, keepdims=True))
    normed = (centred * lax.rsqrt(variance + 1e-06) * (1.0 + temporal_scale) + temporal_shift).astype(jnp.bfloat16)
    packed = jnp.dot(normed, temporal_weight, preferred_element_type=jnp.float32).astype(jnp.bfloat16)
    packed = jnp.transpose(packed.reshape(FRAMES, PATCHES, 3 * D), (1, 0, 2))
    ends = jnp.cumsum(clip_lengths.astype(jnp.int32))
    clip_of = lax.optimization_barrier(jnp.sum((jnp.arange(FRAMES, dtype=jnp.int32)[:, None] >= ends[None, :]).astype(jnp.int32), axis=1))
    allowed = clip_of[:, None] == clip_of[None, :]

    def one_position(rows):
        split = (FRAMES, HEADS, head_dim)
        query = rows[:, :D].reshape(split)
        keys = rows[:, D:2 * D].reshape(split)
        values = rows[:, 2 * D:].reshape(split)
        return attend(query, keys, values, allowed).reshape(FRAMES, D)
    temporal = lax.map(one_position, packed)
    temporal_out = jnp.transpose(temporal, (1, 0, 2))
    return (hidden.reshape(FRAMES, PATCHES, D), temporal_out)
```

```python
import math

import jax
import jax.numpy as jnp
from jax import lax
from jax.experimental import pallas as pl
from jax.experimental.pallas import tpu as pltpu
from jax.sharding import PartitionSpec as P

MESH = pl.DeviceIdType.MESH
BF = jnp.bfloat16
F32 = jnp.float32

HEADS = 16
HD = 72
D = HEADS * HD
NS = 16
NF = 32
ROWS = 64
NZ = 8
SHARD = 36
QUAD = 4 * SHARD
HALF = D // 2
WT = 3 * HALF
GROUP = 4
TOK = NF * GROUP
NEG = -1e30
LOG2E = 1.4426950408889634

ORDER = tuple((j % 2) * 8 + j // 2 for j in range(HEADS))


def remote(src, dst, send, recv, f, s):
    return pltpu.make_async_remote_copy(
        src_ref=src, dst_ref=dst, send_sem=send, recv_sem=recv, device_id=(f, s), device_id_type=MESH
    )


def kernel(
    clip_ref, q_ref, k_ref, v_ref, lat_ref, wp_ref, wt_ref, bias_ref, gate_ref, shift_ref, scale_ref,
    hidden_ref, out_ref,
    pack, got, att, attgot, wpq, wtq, wp, wt, toks, tokgot, rets, retgot, flat, mask_ref,
    qkv_s, qkv_r, att_s, att_r, tok_s, tok_r, ret_s, ret_r,
    pre_s, pre_r, ring_s, ring_r, die_s, die_r,
):
    f = lax.axis_index("frame")
    s = lax.axis_index("space")
    row = f // 16
    z = (f // 2) % NZ
    c = f % 2
    group = f % 16
    yhi = s % 4
    step = 1 - 2 * c
    fz = row * 16 + ((z + step + NZ) % NZ) * 2 + c
    sib = row * 16 + z * 2 + (1 - c)
    other = (1 - row) * 16 + z * 2 + c
    sb = (s - yhi) + (yhi + 2 * row - 1 + 4) % 4
    me_q = row * 2 + c
    other_q = (1 - row) * 2 + c

    barrier = pltpu.get_barrier_semaphore()

    def hail_space(i, _):
        pl.semaphore_signal(barrier, inc=1, device_id=(f, (s + i) % NS), device_id_type=MESH)
        return 0

    def hail_frame(i, _):
        pl.semaphore_signal(barrier, inc=1, device_id=((f + i) % NF, s), device_id_type=MESH)
        return 0

    lax.fori_loop(1, NS, hail_space, 0)
    lax.fori_loop(1, NF, hail_frame, 0)
    pl.semaphore_signal(barrier, inc=1, device_id=(other, sb), device_id_type=MESH)

    for h in range(HEADS):
        cut = pl.ds(h * HD, HD)
        kk, qq, vv = k_ref[:, cut], q_ref[:, cut], v_ref[:, cut]
        pack[h, :, 0:128] = jnp.concatenate([kk, qq[:, :56]], axis=1)
        pack[h, :, 128:256] = jnp.concatenate([vv, qq[:, 56:], jnp.zeros((ROWS, 40), BF)], axis=1)
    wpq[me_q] = wp_ref[...]
    wtq[me_q] = wt_ref[row]

    pl.semaphore_wait(barrier, NS - 1 + NF - 1 + 1)

    wp_y = remote(wp_ref, wpq.at[me_q], pre_s.at[0], pre_r.at[0], other, sb)
    wp_c = remote(wp_ref, wpq.at[me_q], pre_s.at[1], pre_r.at[1], sib, s)
    wp_y.start()
    wp_c.start()

    def send_qkv(i, _):
        to = (s + i) % NS
        remote(pack.at[to], got.at[s], qkv_s, qkv_r, f, to).start()
        return 0

    lax.fori_loop(1, NS, send_qkv, 0)
    wt_y = remote(wt_ref.at[1 - row], wtq.at[me_q], pre_s.at[2], pre_r.at[2], other, s)
    wt_c = remote(wt_ref.at[row], wtq.at[me_q], pre_s.at[3], pre_r.at[3], sib, s)
    wt_y.start()
    wt_c.start()
    got[s] = pack[s]

    def ring(m, buf, k):
        block = (z - step * k + 2 * NZ) % NZ
        src = buf.at[block] if k < 3 else buf.at[block, pl.ds(pl.multiple_of(c * 64, 16), 80)]
        return remote(src, src, ring_s.at[m * 4 + k], ring_r.at[m * 4 + k], fz, s)

    def ring_arrived(m, buf, k):
        block = (z - step * (k + 1) + 2 * NZ) % NZ
        dst = buf.at[block] if k < 3 else buf.at[block, pl.ds(pl.multiple_of(c * 64, 16), 80)]
        return remote(dst, dst, ring_s.at[m * 4 + k], ring_r.at[m * 4 + k], fz, s)

    def die(m, buf, k):
        block = (z - step * (k + 1) + 2 * NZ) % NZ
        src = buf.at[block] if k < 3 else buf.at[block, pl.ds(pl.multiple_of(c * 80, 16), 64)]
        return remote(src, src, die_s.at[m * 4 + k], die_r.at[m * 4 + k], sib, s)

    def die_arrived(m, buf, k):
        block = (z + step * (k + 1) + 2 * NZ) % NZ
        dst = buf.at[block] if k < 3 else buf.at[block, pl.ds(pl.multiple_of((1 - c) * 80, 16), 64)]
        return remote(dst, dst, die_s.at[m * 4 + k], die_r.at[m * 4 + k], sib, s)

    def relay(m, buf, k):
        ring_arrived(m, buf, k).wait_recv()
        if k < 3:
            ring(m, buf, k + 1).start()
        die(m, buf, k).start()

    def begin(m, quads, buf, over_y, over_c):
        over_y.wait_recv()
        more = remote(quads.at[other_q], quads.at[other_q], pre_s.at[4 + m], pre_r.at[4 + m], sib, s)
        more.start()
        over_c.wait_recv()
        more.wait_recv()
        buf[z] = jnp.concatenate([quads[i].astype(F32) for i in range(4)], axis=0).astype(BF)
        ring(m, buf, 0).start()
        return more

    wp_more = begin(0, wpq, wp, wp_y, wp_c)

    ri = lax.broadcasted_iota(jnp.int32, (TOK, TOK), 0)
    ci = lax.broadcasted_iota(jnp.int32, (TOK, TOK), 1)
    clip_r = jnp.zeros((TOK, TOK), jnp.int32)
    clip_c = jnp.zeros((TOK, TOK), jnp.int32)
    end = jnp.int32(0)
    for i in range(clip_ref.shape[0]):
        end = end + clip_ref[i]
        clip_r = clip_r + jnp.where(ri >= GROUP * end, 1, 0)
        clip_c = clip_c + jnp.where(ci >= GROUP * end, 1, 0)
    same = (clip_r == clip_c) & ((ri % GROUP) == (ci % GROUP))
    mask_ref[...] = jnp.where(same, 1.0, 0.0)

    relay(0, wp, 0)

    def total(buf, n, recv):
        return remote(buf.at[pl.ds(0, n)], buf.at[pl.ds(0, n)], recv, recv, f, s)

    total(got, NS - 1, qkv_r).wait_recv()

    lane = lax.broadcasted_iota(jnp.int32, (NS * ROWS, 128), 1)
    left = got[:, :, 0:128].reshape(NS * ROWS, 128)
    right = got[:, :, 128:256].reshape(NS * ROWS, 128)
    values = jnp.where(lane < HD, right.astype(F32), jnp.where(lane == HD, 1.0, 0.0)).astype(BF)
    qblock = 256
    factor = LOG2E / math.sqrt(HD)
    qlane = lax.broadcasted_iota(jnp.int32, (qblock, 128), 1)

    for i in range(NS * ROWS // qblock):
        lo = left[i * qblock : (i + 1) * qblock].astype(F32)
        hi = right[i * qblock : (i + 1) * qblock].astype(F32)
        query = jnp.where(
            qlane < 56, pltpu.roll(lo, 56, 1), jnp.where(qlane < HD, pltpu.roll(hi, 112, 1), 0.0)
        ).astype(BF)
        scores = lax.dot_general(query, left, (((1,), (1,)), ((), ())), preferred_element_type=F32)
        top = jnp.max(scores, axis=1, keepdims=True)
        probs = jnp.exp2((scores - top) * factor).astype(BF)
        mixed = jnp.dot(probs, values, preferred_element_type=F32)
        mixed = (mixed / mixed[:, HD : HD + 1]).astype(BF)
        each = qblock // ROWS
        att[pl.ds(i * each, each)] = mixed.reshape(each, ROWS, 128)
        for j in range(each):
            to = i * each + j

            @pl.when(s != to)
            def _():
                remote(att.at[to], attgot.at[s], att_s, att_r, f, to).start()

        if i == 1:
            relay(0, wp, 1)
    attgot[s] = att[s]

    relay(0, wp, 2)
    wt_more = begin(1, wtq, wt, wt_y, wt_c)
    ring_arrived(0, wp, 3).wait_recv()
    die(0, wp, 3).start()

    total(attgot, NS - 1, att_r).wait_recv()
    rows = jnp.concatenate([attgot[h, :, 0:HD] for h in ORDER], axis=1)
    for k in range(4):
        die_arrived(0, wp, k).wait_recv()
    projected = jnp.dot(rows, wp[...].reshape(D, D), preferred_element_type=F32)
    hidden = lat_ref[...].astype(F32) + gate_ref[...] * (projected + bias_ref[...])
    hidden_ref[...] = hidden
    mean = jnp.mean(hidden, axis=1, keepdims=True)
    centred = hidden - mean
    variance = jnp.mean(centred * centred, axis=1, keepdims=True)
    flat[...] = centred * lax.rsqrt(variance + 1e-06) * (1.0 + scale_ref[...]) + shift_ref[...]
    normed = jnp.concatenate([flat[:, pl.ds(h * HD, HD)] for h in ORDER], axis=1)
    for g in range(ROWS // GROUP):
        toks[g] = normed[g * GROUP : (g + 1) * GROUP].astype(BF)

    def send_tok(i, _):
        to = (f + i) % NF
        remote(toks.at[to % 16], tokgot.at[f], tok_s, tok_r, to, s).start()
        return 0

    lax.fori_loop(1, NF, send_tok, 0)
    tokgot[f] = toks[group]

    for k in range(3):
        relay(1, wt, k)
    ring_arrived(1, wt, 3).wait_recv()
    die(1, wt, 3).start()
    total(tokgot, NF - 1, tok_r).wait_recv()
    x = jnp.concatenate([tokgot[i].astype(F32) for i in range(NF)], axis=0).astype(BF)
    for k in range(4):
        die_arrived(1, wt, k).wait_recv()
    packed = jnp.dot(x, wt[...].reshape(D, WT), preferred_element_type=F32).astype(BF)
    allowed = mask_ref[...] > 0.5
    parts = []
    for h in range(HEADS // 2):
        qh = packed[:, h * HD : (h + 1) * HD]
        kh = packed[:, HALF + h * HD : HALF + (h + 1) * HD]
        vh = packed[:, 2 * HALF + h * HD : 2 * HALF + (h + 1) * HD]
        scores = lax.dot_general(qh, kh, (((1,), (1,)), ((), ())), preferred_element_type=F32)
        scores = jnp.where(allowed, scores * (1.0 / math.sqrt(HD)), NEG)
        top = jnp.max(scores, axis=1, keepdims=True)
        probs = jnp.exp(scores - top)
        whole = jnp.sum(probs, axis=1, keepdims=True)
        parts.append(jnp.dot(probs.astype(BF), vh, preferred_element_type=F32) / whole)
    mixed = jnp.concatenate(parts, axis=1)
    for i in range(NF):
        rets[i] = mixed[i * GROUP : (i + 1) * GROUP].astype(BF)

    def send_ret(i, _):
        to = (f + i) % NF
        remote(rets.at[to], retgot.at[f], ret_s, ret_r, to, s).start()
        return 0

    lax.fori_loop(1, NF, send_ret, 0)
    retgot[f] = rets[f]

    for copy in (wp_y, wp_c, wt_y, wt_c, wp_more, wt_more):
        copy.wait_send()
    for m, buf in ((0, wp), (1, wt)):
        for k in range(4):
            ring(m, buf, k).wait_send()
            die(m, buf, k).wait_send()
    total(pack, NS - 1, qkv_s).wait_send()
    total(att, NS - 1, att_s).wait_send()
    for i in range(2):
        n = 16 if i == 0 else 15
        remote(toks.at[pl.ds(0, n)], toks.at[pl.ds(0, n)], tok_s, tok_s, f, s).wait_send()
    total(rets, NF - 1, ret_s).wait_send()

    total(retgot, NF - 1, ret_r).wait_recv()
    out_ref[...] = retgot[...]


def shards(q, k, v, lat, wp, bias, gate, shift, scale, wt, clips):
    wt_halves = jnp.transpose(wt.reshape(SHARD, 3, 2, HALF), (2, 0, 1, 3)).reshape(2, SHARD, WT)
    flat2 = lambda a: a.reshape(ROWS, D)
    vec = lambda a: a.reshape(1, D)
    vmem = pl.BlockSpec(memory_space=pltpu.VMEM)
    hidden, got = pl.pallas_call(
        kernel,
        out_shape=(
            jax.ShapeDtypeStruct((ROWS, D), F32),
            jax.ShapeDtypeStruct((NF, GROUP, HALF), BF),
        ),
        in_specs=[pl.BlockSpec(memory_space=pltpu.SMEM)] + [vmem] * 10,
        out_specs=(vmem, vmem),
        scratch_shapes=[
            pltpu.VMEM((NS, ROWS, 256), BF),
            pltpu.VMEM((NS, ROWS, 256), BF),
            pltpu.VMEM((NS, ROWS, 128), BF),
            pltpu.VMEM((NS, ROWS, 128), BF),
            pltpu.VMEM((4, SHARD, D), BF),
            pltpu.VMEM((4, SHARD, WT), BF),
            pltpu.VMEM((NZ, QUAD, D), BF),
            pltpu.VMEM((NZ, QUAD, WT), BF),
            pltpu.VMEM((ROWS // GROUP, GROUP, D), BF),
            pltpu.VMEM((NF, GROUP, D), BF),
            pltpu.VMEM((NF, GROUP, HALF), BF),
            pltpu.VMEM((NF, GROUP, HALF), BF),
            pltpu.VMEM((ROWS, D), F32),
            pltpu.VMEM((TOK, TOK), F32),
        ]
        + [pltpu.SemaphoreType.DMA] * 8
        + [
            pltpu.SemaphoreType.DMA((6,)),
            pltpu.SemaphoreType.DMA((6,)),
            pltpu.SemaphoreType.DMA((8,)),
            pltpu.SemaphoreType.DMA((8,)),
            pltpu.SemaphoreType.DMA((8,)),
            pltpu.SemaphoreType.DMA((8,)),
        ],
        compiler_params=pltpu.CompilerParams(
            collective_id=0, has_side_effects=True, vmem_limit_bytes=56 * 1024 * 1024
        ),
        name="stdit",
    )(clips, flat2(q), flat2(k), flat2(v), flat2(lat), wp, wt_halves, vec(bias), vec(gate), vec(shift), vec(scale))
    temporal = jnp.transpose(got.reshape(2, 16, GROUP, HALF), (1, 2, 0, 3)).reshape(1, ROWS, D)
    return hidden.reshape(1, ROWS, D), temporal.astype(F32)


def solution(mesh):
    both = P("frame", "space", None)
    return jax.shard_map(
        shards,
        mesh=mesh,
        in_specs=(both, both, both, both, P("frame", None), P(), P(), P(), P(), P("frame", None), P()),
        out_specs=(both, both),
        check_vma=False,
    )
```

```python
import math

import jax
import jax.numpy as jnp
from jax import lax
from jax.experimental import pallas as pl
from jax.experimental.pallas import tpu as pltpu
from jax.sharding import PartitionSpec as P

MESH = pl.DeviceIdType.MESH
BF = jnp.bfloat16
F32 = jnp.float32

HEADS = 16
HD = 72
D = HEADS * HD
NS = 16
NF = 32
ROWS = 64
NZ = 8
SHARD = 36
QUAD = 4 * SHARD
HALF = D // 2
WT = 3 * HALF
GROUP = 4
TOK = NF * GROUP
NEG = -1e30
LOG2E = 1.4426950408889634
CHUNKS = (
    ((0, 384), (384, 384), (768, 384)),
    ((0, 640), (640, 640), (1280, 448)),
)
NC = 3

ORDER = tuple((j % 2) * 8 + j // 2 for j in range(HEADS))


def remote(src, dst, send, recv, f, s):
    return pltpu.make_async_remote_copy(
        src_ref=src, dst_ref=dst, send_sem=send, recv_sem=recv, device_id=(f, s), device_id_type=MESH
    )


def kernel(
    clip_ref, q_ref, k_ref, v_ref, lat_ref, wp_ref, wt_ref, bias_ref, gate_ref, shift_ref, scale_ref,
    hidden_ref, out_ref,
    pack, got, att, attgot, wpq, wtq, wp, wt, toks, tokgot, rets, retgot, flat, mask_ref, wto,
    qkv_s, qkv_r, att_s, att_r, tok_s, tok_r, ret_s, ret_r,
    pre_s, pre_r, ring_s, ring_r, die_s, die_r,
):
    f = lax.axis_index("frame")
    s = lax.axis_index("space")
    row = f // 16
    z = (f // 2) % NZ
    c = f % 2
    group = f % 16
    yhi = s % 4
    step = 1 - 2 * c
    fz = row * 16 + ((z + step + NZ) % NZ) * 2 + c
    sib = row * 16 + z * 2 + (1 - c)
    other = (1 - row) * 16 + z * 2 + c
    sb = (s - yhi) + (yhi + 2 * row - 1 + 4) % 4
    me_q = row * 2 + c
    other_q = (1 - row) * 2 + c

    barrier = pltpu.get_barrier_semaphore()

    def hail_space(i, _):
        pl.semaphore_signal(barrier, inc=1, device_id=(f, (s + i) % NS), device_id_type=MESH)
        return 0

    def hail_frame(i, _):
        pl.semaphore_signal(barrier, inc=1, device_id=((f + i) % NF, s), device_id_type=MESH)
        return 0

    lax.fori_loop(1, NS, hail_space, 0)
    lax.fori_loop(1, NF, hail_frame, 0)
    pl.semaphore_signal(barrier, inc=1, device_id=(other, sb), device_id_type=MESH)

    for h in range(HEADS):
        cut = pl.ds(h * HD, HD)
        kk, qq, vv = k_ref[:, cut], q_ref[:, cut], v_ref[:, cut]
        pack[h, :, 0:128] = jnp.concatenate([kk, qq[:, :56]], axis=1)
        pack[h, :, 128:256] = jnp.concatenate([vv, qq[:, 56:], jnp.zeros((ROWS, 40), BF)], axis=1)
    wpq[me_q] = wp_ref[...]
    for r in range(2):

        @pl.when(row == r)
        def _():
            mine = [wt_ref[:, pl.ds(t * D + r * HALF, HALF)] for t in range(3)]
            rest = [wt_ref[:, pl.ds(t * D + (1 - r) * HALF, HALF)] for t in range(3)]
            wtq[me_q] = jnp.concatenate(mine, axis=1)
            wto[...] = jnp.concatenate(rest, axis=1)

    pl.semaphore_wait(barrier, NS - 1 + NF - 1 + 1)

    wp_y = remote(wp_ref, wpq.at[me_q], pre_s.at[0], pre_r.at[0], other, sb)
    wp_c = remote(wp_ref, wpq.at[me_q], pre_s.at[1], pre_r.at[1], sib, s)
    wp_y.start()
    wp_c.start()

    def send_qkv(i, _):
        to = (s + i) % NS
        remote(pack.at[to], got.at[s], qkv_s, qkv_r, f, to).start()
        return 0

    lax.fori_loop(1, NS, send_qkv, 0)
    wt_y = remote(wto, wtq.at[me_q], pre_s.at[2], pre_r.at[2], other, s)
    wt_c = remote(wtq.at[me_q], wtq.at[me_q], pre_s.at[3], pre_r.at[3], sib, s)
    wt_y.start()
    wt_c.start()
    got[s] = pack[s]

    def piece(m, buf, block, k, first, rows, n):
        cut = pl.ds(*CHUNKS[m][n])
        block = (block + 2 * NZ) % NZ
        if k < 3:
            return buf.at[block, :, cut]
        return buf.at[block, pl.ds(pl.multiple_of(first, 16), rows), cut]

    def ring(m, buf, k, n):
        src = piece(m, buf, z - step * k, k, c * 64, 80, n)
        at = (m * 4 + k) * NC + n
        return remote(src, src, ring_s.at[at], ring_r.at[at], fz, s)

    def ring_arrived(m, buf, k, n):
        dst = piece(m, buf, z - step * (k + 1), k, c * 64, 80, n)
        at = (m * 4 + k) * NC + n
        return remote(dst, dst, ring_s.at[at], ring_r.at[at], fz, s)

    def die(m, buf, k, n):
        src = piece(m, buf, z - step * (k + 1), k, c * 80, 64, n)
        at = (m * 4 + k) * NC + n
        return remote(src, src, die_s.at[at], die_r.at[at], sib, s)

    def die_arrived(m, buf, k, n):
        dst = piece(m, buf, z + step * (k + 1), k, (1 - c) * 80, 64, n)
        at = (m * 4 + k) * NC + n
        return remote(dst, dst, die_s.at[at], die_r.at[at], sib, s)

    def relay(m, buf, k, chunks=range(NC)):
        for n in chunks:
            ring_arrived(m, buf, k, n).wait_recv()
            if k < 3:
                ring(m, buf, k + 1, n).start()
            die(m, buf, k, n).start()

    def begin(m, quads, buf, over_y, over_c):
        over_y.wait_recv()
        more = remote(quads.at[other_q], quads.at[other_q], pre_s.at[4 + m], pre_r.at[4 + m], sib, s)
        more.start()
        over_c.wait_recv()
        more.wait_recv()
        buf[z] = jnp.concatenate([quads[i].astype(F32) for i in range(4)], axis=0).astype(BF)
        for n in range(NC):
            ring(m, buf, 0, n).start()
        return more

    wp_more = begin(0, wpq, wp, wp_y, wp_c)

    ri = lax.broadcasted_iota(jnp.int32, (TOK, TOK), 0)
    ci = lax.broadcasted_iota(jnp.int32, (TOK, TOK), 1)
    clip_r = jnp.zeros((TOK, TOK), jnp.int32)
    clip_c = jnp.zeros((TOK, TOK), jnp.int32)
    end = jnp.int32(0)
    for i in range(clip_ref.shape[0]):
        end = end + clip_ref[i]
        clip_r = clip_r + jnp.where(ri >= GROUP * end, 1, 0)
        clip_c = clip_c + jnp.where(ci >= GROUP * end, 1, 0)
    same = (clip_r == clip_c) & ((ri % GROUP) == (ci % GROUP))
    mask_ref[...] = jnp.where(same, 1.0, 0.0)

    relay(0, wp, 0)
    relay(0, wp, 1)

    def total(buf, n, recv):
        return remote(buf.at[pl.ds(0, n)], buf.at[pl.ds(0, n)], recv, recv, f, s)

    total(got, NS - 1, qkv_r).wait_recv()

    lane = lax.broadcasted_iota(jnp.int32, (NS * ROWS, 128), 1)
    left = got[:, :, 0:128].reshape(NS * ROWS, 128)
    right = got[:, :, 128:256].reshape(NS * ROWS, 128)
    values = jnp.where(lane < HD, right.astype(F32), jnp.where(lane == HD, 1.0, 0.0)).astype(BF)
    qblock = 256
    factor = LOG2E / math.sqrt(HD)
    qlane = lax.broadcasted_iota(jnp.int32, (qblock, 128), 1)

    for i in range(NS * ROWS // qblock):
        lo = left[i * qblock : (i + 1) * qblock].astype(F32)
        hi = right[i * qblock : (i + 1) * qblock].astype(F32)
        query = jnp.where(
            qlane < 56, pltpu.roll(lo, 56, 1), jnp.where(qlane < HD, pltpu.roll(hi, 112, 1), 0.0)
        ).astype(BF)
        scores = lax.dot_general(query, left, (((1,), (1,)), ((), ())), preferred_element_type=F32)
        top = jnp.max(scores, axis=1, keepdims=True)
        probs = jnp.exp2((scores - top) * factor).astype(BF)
        mixed = jnp.dot(probs, values, preferred_element_type=F32)
        mixed = (mixed / mixed[:, HD : HD + 1]).astype(BF)
        each = qblock // ROWS
        att[pl.ds(i * each, each)] = mixed.reshape(each, ROWS, 128)
        for j in range(each):
            to = i * each + j

            @pl.when(s != to)
            def _():
                remote(att.at[to], attgot.at[s], att_s, att_r, f, to).start()

        if i == 0:
            relay(0, wp, 2)
        if i == 1:
            relay(0, wp, 3)
            wt_more = begin(1, wtq, wt, wt_y, wt_c)
        if i == 3:
            relay(1, wt, 0)
    attgot[s] = att[s]

    total(attgot, NS - 1, att_r).wait_recv()
    rows = jnp.concatenate([attgot[h, :, 0:HD] for h in ORDER], axis=1)
    for k in range(4):
        for n in range(NC):
            die_arrived(0, wp, k, n).wait_recv()
    relay(1, wt, 1)
    projected = jnp.dot(rows, wp[...].reshape(D, D), preferred_element_type=F32)
    hidden = lat_ref[...].astype(F32) + gate_ref[...] * (projected + bias_ref[...])
    hidden_ref[...] = hidden
    mean = jnp.mean(hidden, axis=1, keepdims=True)
    centred = hidden - mean
    variance = jnp.mean(centred * centred, axis=1, keepdims=True)
    flat[...] = centred * lax.rsqrt(variance + 1e-06) * (1.0 + scale_ref[...]) + shift_ref[...]
    normed = jnp.concatenate([flat[:, pl.ds(h * HD, HD)] for h in ORDER], axis=1)
    for g in range(ROWS // GROUP):
        toks[g] = normed[g * GROUP : (g + 1) * GROUP].astype(BF)

    def send_tok(i, _):
        to = (f + i) % NF
        remote(toks.at[to % 16], tokgot.at[f], tok_s, tok_r, to, s).start()
        return 0

    lax.fori_loop(1, NF, send_tok, 0)
    tokgot[f] = toks[group]

    relay(1, wt, 2)
    relay(1, wt, 3)
    total(tokgot, NF - 1, tok_r).wait_recv()
    x = jnp.concatenate([tokgot[i].astype(F32) for i in range(NF)], axis=0).astype(BF)
    for k in range(4):
        for n in range(NC):
            die_arrived(1, wt, k, n).wait_recv()
    packed = jnp.dot(x, wt[...].reshape(D, WT), preferred_element_type=F32).astype(BF)
    allowed = mask_ref[...] > 0.5
    parts = []
    for h in range(HEADS // 2):
        qh = packed[:, h * HD : (h + 1) * HD]
        kh = packed[:, HALF + h * HD : HALF + (h + 1) * HD]
        vh = packed[:, 2 * HALF + h * HD : 2 * HALF + (h + 1) * HD]
        scores = lax.dot_general(qh, kh, (((1,), (1,)), ((), ())), preferred_element_type=F32)
        scores = jnp.where(allowed, scores * (1.0 / math.sqrt(HD)), NEG)
        top = jnp.max(scores, axis=1, keepdims=True)
        probs = jnp.exp(scores - top)
        whole = jnp.sum(probs, axis=1, keepdims=True)
        parts.append(jnp.dot(probs.astype(BF), vh, preferred_element_type=F32) / whole)
    mixed = jnp.concatenate(parts, axis=1)
    for i in range(NF):
        rets[i] = mixed[i * GROUP : (i + 1) * GROUP].astype(BF)

    def send_ret(i, _):
        to = (f + i) % NF
        remote(rets.at[to], retgot.at[f], ret_s, ret_r, to, s).start()
        return 0

    lax.fori_loop(1, NF, send_ret, 0)
    retgot[f] = rets[f]

    for copy in (wp_y, wp_c, wt_y, wt_c, wp_more, wt_more):
        copy.wait_send()
    for m, buf in ((0, wp), (1, wt)):
        for k in range(4):
            for n in range(NC):
                ring(m, buf, k, n).wait_send()
                die(m, buf, k, n).wait_send()
    total(pack, NS - 1, qkv_s).wait_send()
    total(att, NS - 1, att_s).wait_send()
    for i in range(2):
        n = 16 if i == 0 else 15
        remote(toks.at[pl.ds(0, n)], toks.at[pl.ds(0, n)], tok_s, tok_s, f, s).wait_send()
    total(rets, NF - 1, ret_s).wait_send()

    total(retgot, NF - 1, ret_r).wait_recv()
    for g in range(0, 16, 2):
        pair = [jnp.concatenate([retgot[i].astype(F32), retgot[16 + i].astype(F32)], axis=1) for i in (g, g + 1)]
        out_ref[pl.ds(g * GROUP, 2 * GROUP), :] = jnp.concatenate(pair, axis=0)


def shards(q, k, v, lat, wp, bias, gate, shift, scale, wt, clips):
    flat2 = lambda a: a.reshape(ROWS, D)
    vmem = pl.BlockSpec(memory_space=pltpu.VMEM)
    hidden, temporal = pl.pallas_call(
        kernel,
        out_shape=(
            jax.ShapeDtypeStruct((ROWS, D), F32),
            jax.ShapeDtypeStruct((ROWS, D), F32),
        ),
        in_specs=[pl.BlockSpec(memory_space=pltpu.SMEM)] + [vmem] * 10,
        out_specs=(vmem, vmem),
        scratch_shapes=[
            pltpu.VMEM((NS, ROWS, 256), BF),
            pltpu.VMEM((NS, ROWS, 256), BF),
            pltpu.VMEM((NS, ROWS, 128), BF),
            pltpu.VMEM((NS, ROWS, 128), BF),
            pltpu.VMEM((4, SHARD, D), BF),
            pltpu.VMEM((4, SHARD, WT), BF),
            pltpu.VMEM((NZ, QUAD, D), BF),
            pltpu.VMEM((NZ, QUAD, WT), BF),
            pltpu.VMEM((ROWS // GROUP, GROUP, D), BF),
            pltpu.VMEM((NF, GROUP, D), BF),
            pltpu.VMEM((NF, GROUP, HALF), BF),
            pltpu.VMEM((NF, GROUP, HALF), BF),
            pltpu.VMEM((ROWS, D), F32),
            pltpu.VMEM((TOK, TOK), F32),
            pltpu.VMEM((SHARD, WT), BF),
        ]
        + [pltpu.SemaphoreType.DMA] * 8
        + [
            pltpu.SemaphoreType.DMA((6,)),
            pltpu.SemaphoreType.DMA((6,)),
            pltpu.SemaphoreType.DMA((8 * NC,)),
            pltpu.SemaphoreType.DMA((8 * NC,)),
            pltpu.SemaphoreType.DMA((8 * NC,)),
            pltpu.SemaphoreType.DMA((8 * NC,)),
        ],
        compiler_params=pltpu.CompilerParams(
            collective_id=0, has_side_effects=True, vmem_limit_bytes=56 * 1024 * 1024
        ),
        name="stdit",
    )(clips, flat2(q), flat2(k), flat2(v), flat2(lat), wp, wt, bias, gate, shift, scale)
    return hidden.reshape(1, ROWS, D), temporal.reshape(1, ROWS, D)


def solution(mesh):
    both = P("frame", "space", None)
    return jax.shard_map(
        shards,
        mesh=mesh,
        in_specs=(both, both, both, both, P("frame", None), P(), P(), P(), P(), P("frame", None), P()),
        out_specs=(both, both),
        check_vma=False,
    )
```

```python
import math

import jax
import jax.numpy as jnp
from jax import lax
from jax.experimental import pallas as pl
from jax.experimental.pallas import tpu as pltpu
from jax.sharding import PartitionSpec as P

MESH = pl.DeviceIdType.MESH
BF = jnp.bfloat16
F32 = jnp.float32

HEADS = 16
HD = 72
D = HEADS * HD
NS = 16
NF = 32
ROWS = 64
NZ = 8
SHARD = 36
QUAD = 4 * SHARD
HALF = D // 2
WT = 3 * HALF
GROUP = 4
TOK = NF * GROUP
NEG = -1e30
LOG2E = 1.4426950408889634
SHARED = ((0, 384), (1024, 704))
SWAPPED = ((384, 384), (0, 512))
NC = 3

ORDER = tuple((j % 2) * 8 + j // 2 for j in range(HEADS))


def remote(src, dst, send, recv, f, s):
    return pltpu.make_async_remote_copy(
        src_ref=src, dst_ref=dst, send_sem=send, recv_sem=recv, device_id=(f, s), device_id_type=MESH
    )


def kernel(
    clip_ref, q_ref, k_ref, v_ref, lat_ref, wp_ref, wt_ref, bias_ref, gate_ref, shift_ref, scale_ref,
    hidden_ref, out_ref,
    pack, got, att, attgot, wpq, wtq, wp, wt, toks, tokgot, rets, retgot, flat, mask_ref, wto,
    qkv_s, qkv_r, att_s, att_r, tok_s, tok_r, ret_s, ret_r,
    pre_s, pre_r, ring_s, ring_r, die_s, die_r, swap_s, swap_r,
):
    f = lax.axis_index("frame")
    s = lax.axis_index("space")
    row = f // 16
    z = (f // 2) % NZ
    c = f % 2
    group = f % 16
    yhi = s % 4
    step = 1 - 2 * c
    fz = row * 16 + ((z + step + NZ) % NZ) * 2 + c
    sib = row * 16 + z * 2 + (1 - c)
    other = (1 - row) * 16 + z * 2 + c
    sb = (s - yhi) + (yhi + 2 * row - 1 + 4) % 4
    me_q = row * 2 + c
    other_q = (1 - row) * 2 + c
    x = s // 4
    part = (x % 2, x // 2)
    beside = (s + 4 * (1 - 2 * (x % 2)), (3 - x) * 4 + yhi)

    barrier = pltpu.get_barrier_semaphore()

    def hail_space(i, _):
        pl.semaphore_signal(barrier, inc=1, device_id=(f, (s + i) % NS), device_id_type=MESH)
        return 0

    def hail_frame(i, _):
        pl.semaphore_signal(barrier, inc=1, device_id=((f + i) % NF, s), device_id_type=MESH)
        return 0

    lax.fori_loop(1, NS, hail_space, 0)
    lax.fori_loop(1, NF, hail_frame, 0)
    pl.semaphore_signal(barrier, inc=1, device_id=(other, sb), device_id_type=MESH)

    for h in range(HEADS):
        cut = pl.ds(h * HD, HD)
        kk, qq, vv = k_ref[:, cut], q_ref[:, cut], v_ref[:, cut]
        pack[h, :, 0:128] = jnp.concatenate([kk, qq[:, :56]], axis=1)
        pack[h, :, 128:256] = jnp.concatenate([vv, qq[:, 56:], jnp.zeros((ROWS, 40), BF)], axis=1)
    wpq[me_q] = wp_ref[...]
    for r in range(2):

        @pl.when(row == r)
        def _():
            mine = [wt_ref[:, pl.ds(t * D + r * HALF, HALF)] for t in range(3)]
            rest = [wt_ref[:, pl.ds(t * D + (1 - r) * HALF, HALF)] for t in range(3)]
            wtq[me_q] = jnp.concatenate(mine, axis=1)
            wto[...] = jnp.concatenate(rest, axis=1)

    pl.semaphore_wait(barrier, NS - 1 + NF - 1 + 1)

    wp_y = remote(wp_ref, wpq.at[me_q], pre_s.at[0], pre_r.at[0], other, sb)
    wp_c = remote(wp_ref, wpq.at[me_q], pre_s.at[1], pre_r.at[1], sib, s)
    wp_y.start()
    wp_c.start()
    wt_y = remote(wto, wtq.at[me_q], pre_s.at[2], pre_r.at[2], other, s)
    wt_c = remote(wtq.at[me_q], wtq.at[me_q], pre_s.at[3], pre_r.at[3], sib, s)
    wt_y.start()
    wt_c.start()

    def send_qkv(i, _):
        to = (s + i) % NS
        remote(pack.at[to], got.at[s], qkv_s, qkv_r, f, to).start()
        return 0

    lax.fori_loop(1, NS, send_qkv, 0)
    got[s] = pack[s]

    def piece(m, buf, block, k, first, rows, n):
        if n == 0:
            cut = pl.ds(*SHARED[m])
        else:
            first_column, width = SWAPPED[m]
            which = part[m] if n == 1 else 1 - part[m]
            cut = pl.ds(pl.multiple_of(first_column + which * width, 128), width)
        block = (block + 2 * NZ) % NZ
        if k < 3:
            return buf.at[block, :, cut]
        return buf.at[block, pl.ds(pl.multiple_of(first, 16), rows), cut]

    def ring(m, buf, k, n):
        src = piece(m, buf, z - step * k, k, c * 64, 80, n)
        at = (m * 4 + k) * NC + n
        return remote(src, src, ring_s.at[at], ring_r.at[at], fz, s)

    def ring_arrived(m, buf, k, n):
        dst = piece(m, buf, z - step * (k + 1), k, c * 64, 80, n)
        at = (m * 4 + k) * NC + n
        return remote(dst, dst, ring_s.at[at], ring_r.at[at], fz, s)

    def die(m, buf, k, n):
        src = piece(m, buf, z - step * (k + 1), k, c * 80, 64, n)
        at = (m * 4 + k) * NC + n
        return remote(src, src, die_s.at[at], die_r.at[at], sib, s)

    def die_arrived(m, buf, k, n):
        dst = piece(m, buf, z + step * (k + 1), k, (1 - c) * 80, 64, n)
        at = (m * 4 + k) * NC + n
        return remote(dst, dst, die_s.at[at], die_r.at[at], sib, s)

    def swap(m, buf, k, n):
        ref = piece(m, buf, z - step * (k + 1), k, c * 64, 80, n)
        return remote(ref, ref, swap_s.at[m * 4 + k], swap_r.at[m * 4 + k], f, beside[m])

    def relay(m, buf, k, chunks=(0, 1)):
        for n in chunks:
            ring_arrived(m, buf, k, n).wait_recv()
            if k < 3:
                ring(m, buf, k + 1, n).start()
            if n == 1:
                swap(m, buf, k, 1).start()
            die(m, buf, k, n).start()

    def swapped(m, buf, k):
        swap(m, buf, k, 2).wait_recv()
        die(m, buf, k, 2).start()

    def begin(m, quads, buf, over_y, over_c):
        over_y.wait_recv()
        more = remote(quads.at[other_q], quads.at[other_q], pre_s.at[4 + m], pre_r.at[4 + m], sib, s)
        more.start()
        over_c.wait_recv()
        more.wait_recv()
        buf[z] = jnp.concatenate([quads[i].astype(F32) for i in range(4)], axis=0).astype(BF)
        for n in range(2 - m):
            ring(m, buf, 0, n).start()
        return more

    wp_more = begin(0, wpq, wp, wp_y, wp_c)
    wt_more = begin(1, wtq, wt, wt_y, wt_c)

    ri = lax.broadcasted_iota(jnp.int32, (TOK, TOK), 0)
    ci = lax.broadcasted_iota(jnp.int32, (TOK, TOK), 1)
    clip_r = jnp.zeros((TOK, TOK), jnp.int32)
    clip_c = jnp.zeros((TOK, TOK), jnp.int32)
    end = jnp.int32(0)
    for i in range(clip_ref.shape[0]):
        end = end + clip_ref[i]
        clip_r = clip_r + jnp.where(ri >= GROUP * end, 1, 0)
        clip_c = clip_c + jnp.where(ci >= GROUP * end, 1, 0)
    same = (clip_r == clip_c) & ((ri % GROUP) == (ci % GROUP))
    mask_ref[...] = jnp.where(same, 1.0, 0.0)

    relay(0, wp, 0)
    ring(1, wt, 0, 1).start()

    def total(buf, n, recv):
        return remote(buf.at[pl.ds(0, n)], buf.at[pl.ds(0, n)], recv, recv, f, s)

    total(got, NS - 1, qkv_r).wait_recv()

    lane = lax.broadcasted_iota(jnp.int32, (NS * ROWS, 128), 1)
    left = got[:, :, 0:128].reshape(NS * ROWS, 128)
    right = got[:, :, 128:256].reshape(NS * ROWS, 128)
    values = jnp.where(lane < HD, right.astype(F32), jnp.where(lane == HD, 1.0, 0.0)).astype(BF)
    qblock = 256
    factor = LOG2E / math.sqrt(HD)
    qlane = lax.broadcasted_iota(jnp.int32, (qblock, 128), 1)

    for i in range(NS * ROWS // qblock):
        lo = left[i * qblock : (i + 1) * qblock].astype(F32)
        hi = right[i * qblock : (i + 1) * qblock].astype(F32)
        query = jnp.where(
            qlane < 56, pltpu.roll(lo, 56, 1), jnp.where(qlane < HD, pltpu.roll(hi, 112, 1), 0.0)
        ).astype(BF)
        scores = lax.dot_general(query, left, (((1,), (1,)), ((), ())), preferred_element_type=F32)
        top = jnp.max(scores, axis=1, keepdims=True)
        probs = jnp.exp2((scores - top) * factor).astype(BF)
        mixed = jnp.dot(probs, values, preferred_element_type=F32)
        mixed = (mixed / mixed[:, HD : HD + 1]).astype(BF)
        each = qblock // ROWS
        att[pl.ds(i * each, each)] = mixed.reshape(each, ROWS, 128)
        for j in range(each):
            to = i * each + j

            @pl.when(s != to)
            def _():
                remote(att.at[to], attgot.at[s], att_s, att_r, f, to).start()

        if i == 1:
            relay(0, wp, 1)
        if i == 3:
            relay(1, wt, 0, (0,))
    attgot[s] = att[s]

    swapped(0, wp, 0)
    relay(0, wp, 2)
    relay(1, wt, 0, (1,))
    swapped(0, wp, 1)
    relay(0, wp, 3)
    relay(1, wt, 1, (0,))
    swapped(0, wp, 2)
    relay(1, wt, 1, (1,))
    swapped(0, wp, 3)

    total(attgot, NS - 1, att_r).wait_recv()
    rows = jnp.concatenate([attgot[h, :, 0:HD] for h in ORDER], axis=1)
    for k in range(4):
        for n in range(NC):
            die_arrived(0, wp, k, n).wait_recv()
    projected = jnp.dot(rows, wp[...].reshape(D, D), preferred_element_type=F32)
    relay(1, wt, 2, (0,))
    hidden = lat_ref[...].astype(F32) + gate_ref[...] * (projected + bias_ref[...])
    hidden_ref[...] = hidden
    mean = jnp.mean(hidden, axis=1, keepdims=True)
    centred = hidden - mean
    variance = jnp.mean(centred * centred, axis=1, keepdims=True)
    flat[...] = centred * lax.rsqrt(variance + 1e-06) * (1.0 + scale_ref[...]) + shift_ref[...]
    normed = jnp.concatenate([flat[:, pl.ds(h * HD, HD)] for h in ORDER], axis=1)
    for g in range(ROWS // GROUP):
        toks[g] = normed[g * GROUP : (g + 1) * GROUP].astype(BF)

    def send_tok(i, _):
        to = (f + i) % NF
        remote(toks.at[to % 16], tokgot.at[f], tok_s, tok_r, to, s).start()
        return 0

    lax.fori_loop(1, NF, send_tok, 0)
    tokgot[f] = toks[group]

    relay(1, wt, 2, (1,))
    swapped(1, wt, 0)
    swapped(1, wt, 1)
    relay(1, wt, 3)
    swapped(1, wt, 2)
    swapped(1, wt, 3)
    total(tokgot, NF - 1, tok_r).wait_recv()
    tokens = jnp.concatenate([tokgot[i].astype(F32) for i in range(NF)], axis=0).astype(BF)
    for k in range(4):
        for n in range(NC):
            die_arrived(1, wt, k, n).wait_recv()
    packed = jnp.dot(tokens, wt[...].reshape(D, WT), preferred_element_type=F32).astype(BF)
    allowed = mask_ref[...] > 0.5
    parts = []
    for h in range(HEADS // 2):
        qh = packed[:, h * HD : (h + 1) * HD]
        kh = packed[:, HALF + h * HD : HALF + (h + 1) * HD]
        vh = packed[:, 2 * HALF + h * HD : 2 * HALF + (h + 1) * HD]
        scores = lax.dot_general(qh, kh, (((1,), (1,)), ((), ())), preferred_element_type=F32)
        scores = jnp.where(allowed, scores * (1.0 / math.sqrt(HD)), NEG)
        top = jnp.max(scores, axis=1, keepdims=True)
        probs = jnp.exp(scores - top)
        whole = jnp.sum(probs, axis=1, keepdims=True)
        parts.append(jnp.dot(probs.astype(BF), vh, preferred_element_type=F32) / whole)
    mixed = jnp.concatenate(parts, axis=1)
    for i in range(NF):
        rets[i] = mixed[i * GROUP : (i + 1) * GROUP].astype(BF)

    def send_ret(i, _):
        to = (f + i) % NF
        remote(rets.at[to], retgot.at[f], ret_s, ret_r, to, s).start()
        return 0

    lax.fori_loop(1, NF, send_ret, 0)
    retgot[f] = rets[f]

    for copy in (wp_y, wp_c, wt_y, wt_c, wp_more, wt_more):
        copy.wait_send()
    for m, buf in ((0, wp), (1, wt)):
        for k in range(4):
            for n in range(NC):
                if n < 2:
                    ring(m, buf, k, n).wait_send()
                die(m, buf, k, n).wait_send()
            swap(m, buf, k, 1).wait_send()
    total(pack, NS - 1, qkv_s).wait_send()
    total(att, NS - 1, att_s).wait_send()
    for i in range(2):
        n = 16 if i == 0 else 15
        remote(toks.at[pl.ds(0, n)], toks.at[pl.ds(0, n)], tok_s, tok_s, f, s).wait_send()
    total(rets, NF - 1, ret_s).wait_send()

    total(retgot, NF - 1, ret_r).wait_recv()
    for g in range(0, 16, 2):
        pair = [jnp.concatenate([retgot[i].astype(F32), retgot[16 + i].astype(F32)], axis=1) for i in (g, g + 1)]
        out_ref[pl.ds(g * GROUP, 2 * GROUP), :] = jnp.concatenate(pair, axis=0)


def shards(q, k, v, lat, wp, bias, gate, shift, scale, wt, clips):
    flat2 = lambda a: a.reshape(ROWS, D)
    vmem = pl.BlockSpec(memory_space=pltpu.VMEM)
    hidden, temporal = pl.pallas_call(
        kernel,
        out_shape=(
            jax.ShapeDtypeStruct((ROWS, D), F32),
            jax.ShapeDtypeStruct((ROWS, D), F32),
        ),
        in_specs=[pl.BlockSpec(memory_space=pltpu.SMEM)] + [vmem] * 10,
        out_specs=(vmem, vmem),
        scratch_shapes=[
            pltpu.VMEM((NS, ROWS, 256), BF),
            pltpu.VMEM((NS, ROWS, 256), BF),
            pltpu.VMEM((NS, ROWS, 128), BF),
            pltpu.VMEM((NS, ROWS, 128), BF),
            pltpu.VMEM((4, SHARD, D), BF),
            pltpu.VMEM((4, SHARD, WT), BF),
            pltpu.VMEM((NZ, QUAD, D), BF),
            pltpu.VMEM((NZ, QUAD, WT), BF),
            pltpu.VMEM((ROWS // GROUP, GROUP, D), BF),
            pltpu.VMEM((NF, GROUP, D), BF),
            pltpu.VMEM((NF, GROUP, HALF), BF),
            pltpu.VMEM((NF, GROUP, HALF), BF),
            pltpu.VMEM((ROWS, D), F32),
            pltpu.VMEM((TOK, TOK), F32),
            pltpu.VMEM((SHARD, WT), BF),
        ]
        + [pltpu.SemaphoreType.DMA] * 8
        + [
            pltpu.SemaphoreType.DMA((6,)),
            pltpu.SemaphoreType.DMA((6,)),
            pltpu.SemaphoreType.DMA((8 * NC,)),
            pltpu.SemaphoreType.DMA((8 * NC,)),
            pltpu.SemaphoreType.DMA((8 * NC,)),
            pltpu.SemaphoreType.DMA((8 * NC,)),
            pltpu.SemaphoreType.DMA((8,)),
            pltpu.SemaphoreType.DMA((8,)),
        ],
        compiler_params=pltpu.CompilerParams(
            collective_id=0, has_side_effects=True, vmem_limit_bytes=56 * 1024 * 1024
        ),
        name="stdit",
    )(clips, flat2(q), flat2(k), flat2(v), flat2(lat), wp, wt, bias, gate, shift, scale)
    return hidden.reshape(1, ROWS, D), temporal.reshape(1, ROWS, D)


def solution(mesh):
    both = P("frame", "space", None)
    return jax.shard_map(
        shards,
        mesh=mesh,
        in_specs=(both, both, both, both, P("frame", None), P(), P(), P(), P(), P("frame", None), P()),
        out_specs=(both, both),
        check_vma=False,
    )
```

```python
import math

import jax
import jax.numpy as jnp
from jax import lax
from jax.experimental import pallas as pl
from jax.experimental.pallas import tpu as pltpu
from jax.sharding import PartitionSpec as P

MESH = pl.DeviceIdType.MESH
BF = jnp.bfloat16
F32 = jnp.float32

HEADS = 16
HD = 72
D = HEADS * HD
NS = 16
NF = 32
ROWS = 64
NZ = 8
SHARD = 36
QUAD = 4 * SHARD
HALF = D // 2
WT = 3 * HALF
GROUP = 4
TOK = NF * GROUP
NEG = -1e30
LOG2E = 1.4426950408889634
WIDE = 14 * 128
RINGED = ((512, 640), (896, 896))
SWAPPED = ((640, 512), (896, 896))
PIECES = (((0, 256), (256, 384)), ((0, 512), (512, 384)))
NC = 2
NP = 2

ORDER = tuple((j % 2) * 8 + j // 2 for j in range(HEADS))


def remote(src, dst, send, recv, f, s):
    return pltpu.make_async_remote_copy(
        src_ref=src, dst_ref=dst, send_sem=send, recv_sem=recv, device_id=(f, s), device_id_type=MESH
    )


def kernel(
    clip_ref, q_in, k_in, v_in, lat_in, wp_in, wt_in, bias_ref, gate_ref, shift_ref, scale_ref,
    hidden_out, temporal_out,
    q_ref, k_ref, v_ref, lat_ref, wp_ref, wt_ref, hidden_ref, out_ref, local,
    pack, got, att, attgot, wpq, wtq, wp, wt, toks, tokgot, rets, retgot, flat, mask_ref, wto,
    qkv_s, qkv_r, att_s, att_r, tok_s, tok_r, ret_s, ret_r,
    pre_s, pre_r, ring_s, ring_r, die_s, die_r, swap_s, swap_r,
):
    f = lax.axis_index("frame")
    s = lax.axis_index("space")
    row = f // 16
    z = (f // 2) % NZ
    c = f % 2
    group = f % 16
    yhi = s % 4
    step = 1 - 2 * c
    fz = row * 16 + ((z + step + NZ) % NZ) * 2 + c
    sib = row * 16 + z * 2 + (1 - c)
    other = (1 - row) * 16 + z * 2 + c
    sb = (s - yhi) + (yhi + 2 * row - 1 + 4) % 4
    me_q = row * 2 + c
    other_q = (1 - row) * 2 + c
    x = s // 4
    part = (x % 2, x // 2)
    beside = (s + 4 * (1 - 2 * (x % 2)), (3 - x) * 4 + yhi)

    loads = [
        pltpu.make_async_copy(src, dst, local.at[i])
        for i, (src, dst) in enumerate(
            ((wp_in, wp_ref), (wt_in, wt_ref), (k_in, k_ref), (q_in, q_ref), (v_in, v_ref), (lat_in, lat_ref))
        )
    ]
    for load in loads:
        load.start()

    barrier = pltpu.get_barrier_semaphore()

    def hail_space(i, _):
        pl.semaphore_signal(barrier, inc=1, device_id=(f, (s + i) % NS), device_id_type=MESH)
        return 0

    def hail_frame(i, _):
        pl.semaphore_signal(barrier, inc=1, device_id=((f + i) % NF, s), device_id_type=MESH)
        return 0

    lax.fori_loop(1, NS, hail_space, 0)
    lax.fori_loop(1, NF, hail_frame, 0)
    pl.semaphore_signal(barrier, inc=1, device_id=(other, sb), device_id_type=MESH)

    for load in loads:
        load.wait()
    for h in range(HEADS):
        cut = pl.ds(h * HD, HD)
        kk, qq, vv = k_ref[:, cut], q_ref[:, cut], v_ref[:, cut]
        pack[h, :, 0:128] = jnp.concatenate([kk, qq[:, :56]], axis=1)
        pack[h, :, 128:256] = jnp.concatenate([vv, qq[:, 56:], jnp.zeros((ROWS, 40), BF)], axis=1)
    wpq[me_q] = wp_ref[...]
    for r in range(2):

        @pl.when(row == r)
        def _():
            mine = [wt_ref[:, pl.ds(t * D + r * HALF, HALF)] for t in range(3)]
            rest = [wt_ref[:, pl.ds(t * D + (1 - r) * HALF, HALF)] for t in range(3)]
            pad = [jnp.zeros((SHARD, WIDE - WT), BF)]
            wtq[me_q] = jnp.concatenate(mine + pad, axis=1)
            wto[...] = jnp.concatenate(rest + pad, axis=1)

    pl.semaphore_wait(barrier, NS - 1 + NF - 1 + 1)

    wp_y = remote(wp_ref, wpq.at[me_q], pre_s.at[0], pre_r.at[0], other, sb)
    wp_c = remote(wp_ref, wpq.at[me_q], pre_s.at[1], pre_r.at[1], sib, s)
    wp_y.start()
    wp_c.start()
    wt_y = remote(wto, wtq.at[me_q], pre_s.at[2], pre_r.at[2], other, s)
    wt_c = remote(wtq.at[me_q], wtq.at[me_q], pre_s.at[3], pre_r.at[3], sib, s)
    wt_y.start()
    wt_c.start()

    def send_qkv(i, _):
        to = (s + i) % NS
        remote(pack.at[to], got.at[s], qkv_s, qkv_r, f, to).start()
        return 0

    lax.fori_loop(1, NS, send_qkv, 0)
    got[s] = pack[s]

    def piece(m, buf, block, k, first, rows, kind, own, skip=0, width=None):
        apart, whole = kind[m]
        which = part[m] if own else 1 - part[m]
        cut = pl.ds(pl.multiple_of(which * apart + skip, 128), width or whole)
        block = (block + 2 * NZ) % NZ
        if k < 3:
            return buf.at[block, :, cut]
        return buf.at[block, pl.ds(pl.multiple_of(first, 16), rows), cut]

    def ring(m, buf, k, i):
        src = piece(m, buf, z - step * k, k, c * 64, 80, RINGED, True, *PIECES[m][i])
        at = (m * 4 + k) * NP + i
        return remote(src, src, ring_s.at[at], ring_r.at[at], fz, s)

    def ring_arrived(m, buf, k, i):
        dst = piece(m, buf, z - step * (k + 1), k, c * 64, 80, RINGED, True, *PIECES[m][i])
        at = (m * 4 + k) * NP + i
        return remote(dst, dst, ring_s.at[at], ring_r.at[at], fz, s)

    def die(m, buf, k, n):
        src = piece(m, buf, z - step * (k + 1), k, c * 80, 64, *((RINGED, True) if n == 0 else (SWAPPED, False)))
        at = (m * 4 + k) * NC + n
        return remote(src, src, die_s.at[at], die_r.at[at], sib, s)

    def die_arrived(m, buf, k, n):
        dst = piece(m, buf, z + step * (k + 1), k, (1 - c) * 80, 64, *((RINGED, True) if n == 0 else (SWAPPED, False)))
        at = (m * 4 + k) * NC + n
        return remote(dst, dst, die_s.at[at], die_r.at[at], sib, s)

    def swap(m, buf, k, n):
        ref = piece(m, buf, z - step * (k + 1), k, c * 64, 80, SWAPPED, n == 1)
        return remote(ref, ref, swap_s.at[m * 4 + k], swap_r.at[m * 4 + k], f, beside[m])

    def relay(m, buf, k):
        for i in range(NP):
            ring_arrived(m, buf, k, i).wait_recv()
            if k < 3:
                ring(m, buf, k + 1, i).start()
        swap(m, buf, k, 1).start()
        die(m, buf, k, 0).start()

    def swapped(m, buf, k):
        swap(m, buf, k, 2).wait_recv()
        die(m, buf, k, 1).start()

    def begin(m, quads, buf, over_y, over_c):
        over_y.wait_recv()
        more = remote(quads.at[other_q], quads.at[other_q], pre_s.at[4 + m], pre_r.at[4 + m], sib, s)
        more.start()
        over_c.wait_recv()
        more.wait_recv()
        buf[z] = jnp.concatenate([quads[i].astype(F32) for i in range(4)], axis=0).astype(BF)
        for i in range(NP):
            ring(m, buf, 0, i).start()
        return more

    wp_more = begin(0, wpq, wp, wp_y, wp_c)

    ri = lax.broadcasted_iota(jnp.int32, (TOK, TOK), 0)
    ci = lax.broadcasted_iota(jnp.int32, (TOK, TOK), 1)
    clip_r = jnp.zeros((TOK, TOK), jnp.int32)
    clip_c = jnp.zeros((TOK, TOK), jnp.int32)
    end = jnp.int32(0)
    for i in range(clip_ref.shape[0]):
        end = end + clip_ref[i]
        clip_r = clip_r + jnp.where(ri >= GROUP * end, 1, 0)
        clip_c = clip_c + jnp.where(ci >= GROUP * end, 1, 0)
    same = (clip_r == clip_c) & ((ri % GROUP) == (ci % GROUP))
    mask_ref[...] = jnp.where(same, 1.0, 0.0)

    wt_more = begin(1, wtq, wt, wt_y, wt_c)
    relay(0, wp, 0)
    relay(1, wt, 0)
    relay(0, wp, 1)

    def total(buf, n, recv):
        return remote(buf.at[pl.ds(0, n)], buf.at[pl.ds(0, n)], recv, recv, f, s)

    total(got, NS - 1, qkv_r).wait_recv()

    lane = lax.broadcasted_iota(jnp.int32, (NS * ROWS, 128), 1)
    left = got[:, :, 0:128].reshape(NS * ROWS, 128)
    right = got[:, :, 128:256].reshape(NS * ROWS, 128)
    values = jnp.where(lane < HD, right.astype(F32), jnp.where(lane == HD, 1.0, 0.0)).astype(BF)
    qblock = 256
    factor = LOG2E / math.sqrt(HD)
    qlane = lax.broadcasted_iota(jnp.int32, (qblock, 128), 1)

    for i in range(NS * ROWS // qblock):
        lo = left[i * qblock : (i + 1) * qblock].astype(F32)
        hi = right[i * qblock : (i + 1) * qblock].astype(F32)
        query = jnp.where(
            qlane < 56, pltpu.roll(lo, 56, 1), jnp.where(qlane < HD, pltpu.roll(hi, 112, 1), 0.0)
        ).astype(BF)
        scores = lax.dot_general(query, left, (((1,), (1,)), ((), ())), preferred_element_type=F32)
        top = jnp.max(scores, axis=1, keepdims=True)
        probs = jnp.exp2((scores - top) * factor).astype(BF)
        mixed = jnp.dot(probs, values, preferred_element_type=F32)
        mixed = (mixed / mixed[:, HD : HD + 1]).astype(BF)
        each = qblock // ROWS
        att[pl.ds(i * each, each)] = mixed.reshape(each, ROWS, 128)
        for j in range(each):
            to = i * each + j

            @pl.when(s != to)
            def _():
                remote(att.at[to], attgot.at[s], att_s, att_r, f, to).start()

        if i == 1:
            relay(1, wt, 1)
        if i == 3:
            relay(0, wp, 2)
    attgot[s] = att[s]

    for k in range(3):
        swapped(0, wp, k)
    relay(0, wp, 3)
    swapped(0, wp, 3)
    relay(1, wt, 2)

    total(attgot, NS - 1, att_r).wait_recv()
    rows = jnp.concatenate([attgot[h, :, 0:HD] for h in ORDER], axis=1)
    for k in range(4):
        for n in range(NC):
            die_arrived(0, wp, k, n).wait_recv()
    projected = jnp.dot(rows, wp[...].reshape(D, D), preferred_element_type=F32)
    hidden = lat_ref[...].astype(F32) + gate_ref[...] * (projected + bias_ref[...])
    hidden_ref[...] = hidden
    keep = pltpu.make_async_copy(hidden_ref, hidden_out, local.at[6])
    keep.start()
    mean = jnp.mean(hidden, axis=1, keepdims=True)
    centred = hidden - mean
    variance = jnp.mean(centred * centred, axis=1, keepdims=True)
    flat[...] = centred * lax.rsqrt(variance + 1e-06) * (1.0 + scale_ref[...]) + shift_ref[...]
    normed = jnp.concatenate([flat[:, pl.ds(h * HD, HD)] for h in ORDER], axis=1)
    for g in range(ROWS // GROUP):
        toks[g] = normed[g * GROUP : (g + 1) * GROUP].astype(BF)

    def send_tok(i, _):
        to = (f + i) % NF
        remote(toks.at[to % 16], tokgot.at[f], tok_s, tok_r, to, s).start()
        return 0

    lax.fori_loop(1, NF, send_tok, 0)
    tokgot[f] = toks[group]

    swapped(1, wt, 0)
    swapped(1, wt, 1)
    relay(1, wt, 3)
    swapped(1, wt, 2)
    swapped(1, wt, 3)
    total(tokgot, NF - 1, tok_r).wait_recv()
    tokens = jnp.concatenate([tokgot[i].astype(F32) for i in range(NF)], axis=0).astype(BF)
    for k in range(4):
        for n in range(NC):
            die_arrived(1, wt, k, n).wait_recv()
    packed = jnp.dot(tokens, wt[...].reshape(D, WIDE), preferred_element_type=F32).astype(BF)
    allowed = mask_ref[...] > 0.5
    parts = []
    for h in range(HEADS // 2):
        qh = packed[:, h * HD : (h + 1) * HD]
        kh = packed[:, HALF + h * HD : HALF + (h + 1) * HD]
        vh = packed[:, 2 * HALF + h * HD : 2 * HALF + (h + 1) * HD]
        scores = lax.dot_general(qh, kh, (((1,), (1,)), ((), ())), preferred_element_type=F32)
        scores = jnp.where(allowed, scores * (1.0 / math.sqrt(HD)), NEG)
        top = jnp.max(scores, axis=1, keepdims=True)
        probs = jnp.exp(scores - top)
        whole = jnp.sum(probs, axis=1, keepdims=True)
        parts.append(jnp.dot(probs.astype(BF), vh, preferred_element_type=F32) / whole)
    mixed = jnp.concatenate(parts, axis=1)
    for i in range(NF):
        rets[i] = mixed[i * GROUP : (i + 1) * GROUP].astype(BF)

    def send_ret(i, _):
        to = (f + i) % NF
        remote(rets.at[to], retgot.at[f], ret_s, ret_r, to, s).start()
        return 0

    lax.fori_loop(1, NF, send_ret, 0)
    retgot[f] = rets[f]

    for copy in (wp_y, wp_c, wt_y, wt_c, wp_more, wt_more):
        copy.wait_send()
    for m, buf in ((0, wp), (1, wt)):
        for k in range(4):
            for i in range(NP):
                ring(m, buf, k, i).wait_send()
            for n in range(NC):
                die(m, buf, k, n).wait_send()
            swap(m, buf, k, 1).wait_send()
    total(pack, NS - 1, qkv_s).wait_send()
    total(att, NS - 1, att_s).wait_send()
    for i in range(2):
        n = 16 if i == 0 else 15
        remote(toks.at[pl.ds(0, n)], toks.at[pl.ds(0, n)], tok_s, tok_s, f, s).wait_send()
    total(rets, NF - 1, ret_s).wait_send()

    total(retgot, NF - 1, ret_r).wait_recv()
    for g in range(0, 16, 2):
        pair = [jnp.concatenate([retgot[i].astype(F32), retgot[16 + i].astype(F32)], axis=1) for i in (g, g + 1)]
        out_ref[pl.ds(g * GROUP, 2 * GROUP), :] = jnp.concatenate(pair, axis=0)
    last = pltpu.make_async_copy(out_ref, temporal_out, local.at[7])
    last.start()
    keep.wait()
    last.wait()


def shards(q, k, v, lat, wp, bias, gate, shift, scale, wt, clips):
    flat2 = lambda a: a.reshape(ROWS, D)
    vmem = pl.BlockSpec(memory_space=pltpu.VMEM)
    hbm = pl.BlockSpec(memory_space=pl.ANY)
    hidden, temporal = pl.pallas_call(
        kernel,
        out_shape=(
            jax.ShapeDtypeStruct((ROWS, D), F32),
            jax.ShapeDtypeStruct((ROWS, D), F32),
        ),
        in_specs=[pl.BlockSpec(memory_space=pltpu.SMEM)] + [hbm] * 6 + [vmem] * 4,
        out_specs=(hbm, hbm),
        scratch_shapes=[
            pltpu.VMEM((ROWS, D), BF),
            pltpu.VMEM((ROWS, D), BF),
            pltpu.VMEM((ROWS, D), BF),
            pltpu.VMEM((ROWS, D), BF),
            pltpu.VMEM((SHARD, D), BF),
            pltpu.VMEM((SHARD, 3 * D), BF),
            pltpu.VMEM((ROWS, D), F32),
            pltpu.VMEM((ROWS, D), F32),
            pltpu.SemaphoreType.DMA((8,)),
            pltpu.VMEM((NS, ROWS, 256), BF),
            pltpu.VMEM((NS, ROWS, 256), BF),
            pltpu.VMEM((NS, ROWS, 128), BF),
            pltpu.VMEM((NS, ROWS, 128), BF),
            pltpu.VMEM((4, SHARD, D), BF),
            pltpu.VMEM((4, SHARD, WIDE), BF),
            pltpu.VMEM((NZ, QUAD, D), BF),
            pltpu.VMEM((NZ, QUAD, WIDE), BF),
            pltpu.VMEM((ROWS // GROUP, GROUP, D), BF),
            pltpu.VMEM((NF, GROUP, D), BF),
            pltpu.VMEM((NF, GROUP, HALF), BF),
            pltpu.VMEM((NF, GROUP, HALF), BF),
            pltpu.VMEM((ROWS, D), F32),
            pltpu.VMEM((TOK, TOK), F32),
            pltpu.VMEM((SHARD, WIDE), BF),
        ]
        + [pltpu.SemaphoreType.DMA] * 8
        + [
            pltpu.SemaphoreType.DMA((6,)),
            pltpu.SemaphoreType.DMA((6,)),
            pltpu.SemaphoreType.DMA((8 * NP,)),
            pltpu.SemaphoreType.DMA((8 * NP,)),
            pltpu.SemaphoreType.DMA((8 * NC,)),
            pltpu.SemaphoreType.DMA((8 * NC,)),
            pltpu.SemaphoreType.DMA((8,)),
            pltpu.SemaphoreType.DMA((8,)),
        ],
        compiler_params=pltpu.CompilerParams(
            collective_id=0, has_side_effects=True, vmem_limit_bytes=56 * 1024 * 1024
        ),
        name="stdit",
    )(clips, flat2(q), flat2(k), flat2(v), flat2(lat), wp, wt, bias, gate, shift, scale)
    return hidden.reshape(1, ROWS, D), temporal.reshape(1, ROWS, D)


def solution(mesh):
    both = P("frame", "space", None)
    return jax.shard_map(
        shards,
        mesh=mesh,
        in_specs=(both, both, both, both, P("frame", None), P(), P(), P(), P(), P("frame", None), P()),
        out_specs=(both, both),
        check_vma=False,
    )
```

```python
import math

import jax
import jax.numpy as jnp
from jax import lax
from jax.experimental import pallas as pl
from jax.experimental.pallas import tpu as pltpu
from jax.sharding import PartitionSpec as P

MESH = pl.DeviceIdType.MESH
BF = jnp.bfloat16
F32 = jnp.float32

HEADS = 16
HD = 72
D = HEADS * HD
NS = 16
NF = 32
ROWS = 64
NZ = 8
SHARD = 36
QUAD = 4 * SHARD
HALF = D // 2
WT = 3 * HALF
GROUP = 4
TOK = NF * GROUP
NEG = -1e30
LOG2E = 1.4426950408889634
WIDE = 14 * 128
RINGED = ((512, 640), (896, 896))
SWAPPED = ((640, 512), (896, 896))
PIECES = (((0, 256), (256, 384)), ((0, 512), (512, 384)))
NC = 2
NP = 2

ORDER = tuple((j % 2) * 8 + j // 2 for j in range(HEADS))


def remote(src, dst, send, recv, f, s):
    return pltpu.make_async_remote_copy(
        src_ref=src, dst_ref=dst, send_sem=send, recv_sem=recv, device_id=(f, s), device_id_type=MESH
    )


def kernel(
    clip_ref, q_in, k_in, v_in, lat_in, wp_in, wt_in, bias_ref, gate_ref, shift_ref, scale_ref,
    hidden_out, temporal_out,
    q_ref, k_ref, v_ref, lat_ref, wp_ref, wt_ref, hidden_ref, out_ref, local,
    pack, got, att, attgot, wpq, wtq, wp, wt, toks, tokgot, rets, retgot, flat, mask_ref, wto,
    qkv_s, qkv_r, att_s, att_r, tok_s, tok_r, ret_s, ret_r,
    pre_s, pre_r, ring_s, ring_r, die_s, die_r, swap_s, swap_r,
):
    f = lax.axis_index("frame")
    s = lax.axis_index("space")
    row = f // 16
    z = (f // 2) % NZ
    c = f % 2
    group = f % 16
    yhi = s % 4
    step = 1 - 2 * c
    fz = row * 16 + ((z + step + NZ) % NZ) * 2 + c
    sib = row * 16 + z * 2 + (1 - c)
    other = (1 - row) * 16 + z * 2 + c
    sb = (s - yhi) + (yhi + 2 * row - 1 + 4) % 4
    me_q = row * 2 + c
    other_q = (1 - row) * 2 + c
    x = s // 4
    part = (x % 2, x // 2)
    beside = (s + 4 * (1 - 2 * (x % 2)), (3 - x) * 4 + yhi)

    loads = [
        pltpu.make_async_copy(src, dst, local.at[i])
        for i, (src, dst) in enumerate(
            ((wp_in, wp_ref), (wt_in, wt_ref), (k_in, k_ref), (q_in, q_ref), (v_in, v_ref), (lat_in, lat_ref))
        )
    ]
    for load in loads:
        load.start()

    barrier = pltpu.get_barrier_semaphore()

    def hail_space(i, _):
        pl.semaphore_signal(barrier, inc=1, device_id=(f, (s + i) % NS), device_id_type=MESH)
        return 0

    def hail_frame(i, _):
        pl.semaphore_signal(barrier, inc=1, device_id=((f + i) % NF, s), device_id_type=MESH)
        return 0

    lax.fori_loop(1, NS, hail_space, 0)
    lax.fori_loop(1, NF, hail_frame, 0)
    pl.semaphore_signal(barrier, inc=1, device_id=(other, sb), device_id_type=MESH)

    for load in loads:
        load.wait()
    for h in range(HEADS):
        cut = pl.ds(h * HD, HD)
        kk, qq, vv = k_ref[:, cut], q_ref[:, cut], v_ref[:, cut]
        pack[h, :, 0:128] = jnp.concatenate([kk, qq[:, :56]], axis=1)
        pack[h, :, 128:256] = jnp.concatenate([vv, qq[:, 56:], jnp.zeros((ROWS, 40), BF)], axis=1)
    wpq[me_q] = wp_ref[...]
    for r in range(2):

        @pl.when(row == r)
        def _():
            mine = [wt_ref[:, pl.ds(t * D + r * HALF, HALF)] for t in range(3)]
            rest = [wt_ref[:, pl.ds(t * D + (1 - r) * HALF, HALF)] for t in range(3)]
            pad = [jnp.zeros((SHARD, WIDE - WT), BF)]
            wtq[me_q] = jnp.concatenate(mine + pad, axis=1)
            wto[...] = jnp.concatenate(rest + pad, axis=1)

    pl.semaphore_wait(barrier, NS - 1 + NF - 1 + 1)

    wp_y = remote(wp_ref, wpq.at[me_q], pre_s.at[0], pre_r.at[0], other, sb)
    wp_c = remote(wp_ref, wpq.at[me_q], pre_s.at[1], pre_r.at[1], sib, s)
    wp_y.start()
    wp_c.start()
    wt_y = remote(wto, wtq.at[me_q], pre_s.at[2], pre_r.at[2], other, s)
    wt_c = remote(wtq.at[me_q], wtq.at[me_q], pre_s.at[3], pre_r.at[3], sib, s)
    wt_y.start()
    wt_c.start()

    def send_qkv(i, _):
        to = (s + i) % NS
        remote(pack.at[to], got.at[s], qkv_s, qkv_r, f, to).start()
        return 0

    lax.fori_loop(1, NS, send_qkv, 0)
    got[s] = pack[s]

    def piece(m, buf, block, k, first, rows, kind, own, skip=0, width=None):
        apart, whole = kind[m]
        which = part[m] if own else 1 - part[m]
        cut = pl.ds(pl.multiple_of(which * apart + skip, 128), width or whole)
        block = (block + 2 * NZ) % NZ
        if k < 3:
            return buf.at[block, :, cut]
        return buf.at[block, pl.ds(pl.multiple_of(first, 16), rows), cut]

    def ring(m, buf, k, i):
        src = piece(m, buf, z - step * k, k, c * 64, 80, RINGED, True, *PIECES[m][i])
        at = (m * 4 + k) * NP + i
        return remote(src, src, ring_s.at[at], ring_r.at[at], fz, s)

    def ring_arrived(m, buf, k, i):
        dst = piece(m, buf, z - step * (k + 1), k, c * 64, 80, RINGED, True, *PIECES[m][i])
        at = (m * 4 + k) * NP + i
        return remote(dst, dst, ring_s.at[at], ring_r.at[at], fz, s)

    def die(m, buf, k, n):
        src = piece(m, buf, z - step * (k + 1), k, c * 80, 64, *((RINGED, True) if n == 0 else (SWAPPED, False)))
        at = (m * 4 + k) * NC + n
        return remote(src, src, die_s.at[at], die_r.at[at], sib, s)

    def die_arrived(m, buf, k, n):
        dst = piece(m, buf, z + step * (k + 1), k, (1 - c) * 80, 64, *((RINGED, True) if n == 0 else (SWAPPED, False)))
        at = (m * 4 + k) * NC + n
        return remote(dst, dst, die_s.at[at], die_r.at[at], sib, s)

    def swap(m, buf, k, n):
        ref = piece(m, buf, z - step * (k + 1), k, c * 64, 80, SWAPPED, n == 1)
        return remote(ref, ref, swap_s.at[m * 4 + k], swap_r.at[m * 4 + k], f, beside[m])

    def relay(m, buf, k):
        for i in range(NP):
            ring_arrived(m, buf, k, i).wait_recv()
            if k < 3:
                ring(m, buf, k + 1, i).start()
        swap(m, buf, k, 1).start()
        die(m, buf, k, 0).start()

    def swapped(m, buf, k):
        swap(m, buf, k, 2).wait_recv()
        die(m, buf, k, 1).start()

    def begin(m, quads, buf, over_y, over_c):
        over_y.wait_recv()
        more = remote(quads.at[other_q], quads.at[other_q], pre_s.at[4 + m], pre_r.at[4 + m], sib, s)
        more.start()
        over_c.wait_recv()
        more.wait_recv()
        buf[z] = jnp.concatenate([quads[i].astype(F32) for i in range(4)], axis=0).astype(BF)
        for i in range(NP):
            ring(m, buf, 0, i).start()
        return more

    wp_more = begin(0, wpq, wp, wp_y, wp_c)

    ri = lax.broadcasted_iota(jnp.int32, (TOK, TOK), 0)
    ci = lax.broadcasted_iota(jnp.int32, (TOK, TOK), 1)
    clip_r = jnp.zeros((TOK, TOK), jnp.int32)
    clip_c = jnp.zeros((TOK, TOK), jnp.int32)
    end = jnp.int32(0)
    for i in range(clip_ref.shape[0]):
        end = end + clip_ref[i]
        clip_r = clip_r + jnp.where(ri >= GROUP * end, 1, 0)
        clip_c = clip_c + jnp.where(ci >= GROUP * end, 1, 0)
    same = (clip_r == clip_c) & ((ri % GROUP) == (ci % GROUP))
    mask_ref[...] = jnp.where(same, 1.0, 0.0)

    wt_more = begin(1, wtq, wt, wt_y, wt_c)
    relay(0, wp, 0)
    relay(1, wt, 0)
    relay(0, wp, 1)

    def total(buf, n, recv):
        return remote(buf.at[pl.ds(0, n)], buf.at[pl.ds(0, n)], recv, recv, f, s)

    total(got, NS - 1, qkv_r).wait_recv()

    lane = lax.broadcasted_iota(jnp.int32, (NS * ROWS, 128), 1)
    left = got[:, :, 0:128].reshape(NS * ROWS, 128)
    right = got[:, :, 128:256].reshape(NS * ROWS, 128)
    values = jnp.where(lane < HD, right.astype(F32), jnp.where(lane == HD, 1.0, 0.0)).astype(BF)
    qblock = 256
    factor = LOG2E / math.sqrt(HD)
    qlane = lax.broadcasted_iota(jnp.int32, (qblock, 128), 1)

    for i in range(NS * ROWS // qblock):
        lo = left[i * qblock : (i + 1) * qblock].astype(F32)
        hi = right[i * qblock : (i + 1) * qblock].astype(F32)
        query = jnp.where(
            qlane < 56, pltpu.roll(lo, 56, 1), jnp.where(qlane < HD, pltpu.roll(hi, 112, 1), 0.0)
        ).astype(BF)
        scores = lax.dot_general(query, left, (((1,), (1,)), ((), ())), preferred_element_type=F32)
        top = jnp.max(scores, axis=1, keepdims=True)
        probs = jnp.exp2((scores - top) * factor).astype(BF)
        mixed = jnp.dot(probs, values, preferred_element_type=F32)
        mixed = (mixed / mixed[:, HD : HD + 1]).astype(BF)
        each = qblock // ROWS
        att[pl.ds(i * each, each)] = mixed.reshape(each, ROWS, 128)
        for j in range(each):
            to = i * each + j

            @pl.when(s != to)
            def _():
                remote(att.at[to], attgot.at[s], att_s, att_r, f, to).start()

        if i == 1:
            relay(1, wt, 1)
        if i == 3:
            relay(0, wp, 2)
    attgot[s] = att[s]

    swapped(0, wp, 0)
    swapped(0, wp, 1)
    relay(0, wp, 3)
    relay(1, wt, 2)
    swapped(0, wp, 2)
    swapped(0, wp, 3)

    total(attgot, NS - 1, att_r).wait_recv()
    rows = jnp.concatenate([attgot[h, :, 0:HD] for h in ORDER], axis=1)
    for k in range(4):
        for n in range(NC):
            die_arrived(0, wp, k, n).wait_recv()
    projected = jnp.dot(rows, wp[...].reshape(D, D), preferred_element_type=F32)
    relay(1, wt, 3)
    hidden = lat_ref[...].astype(F32) + gate_ref[...] * (projected + bias_ref[...])
    hidden_ref[...] = hidden
    keep = pltpu.make_async_copy(hidden_ref, hidden_out, local.at[6])
    keep.start()
    mean = jnp.mean(hidden, axis=1, keepdims=True)
    centred = hidden - mean
    variance = jnp.mean(centred * centred, axis=1, keepdims=True)
    flat[...] = centred * lax.rsqrt(variance + 1e-06) * (1.0 + scale_ref[...]) + shift_ref[...]
    normed = jnp.concatenate([flat[:, pl.ds(h * HD, HD)] for h in ORDER], axis=1)
    for g in range(ROWS // GROUP):
        toks[g] = normed[g * GROUP : (g + 1) * GROUP].astype(BF)

    def send_tok(i, _):
        to = (f + i) % NF
        remote(toks.at[to % 16], tokgot.at[f], tok_s, tok_r, to, s).start()
        return 0

    lax.fori_loop(1, NF, send_tok, 0)
    tokgot[f] = toks[group]

    swapped(1, wt, 0)
    swapped(1, wt, 1)
    swapped(1, wt, 2)
    swapped(1, wt, 3)
    total(tokgot, NF - 1, tok_r).wait_recv()
    tokens = jnp.concatenate([tokgot[i].astype(F32) for i in range(NF)], axis=0).astype(BF)
    for k in range(4):
        for n in range(NC):
            die_arrived(1, wt, k, n).wait_recv()
    packed = jnp.dot(tokens, wt[...].reshape(D, WIDE), preferred_element_type=F32).astype(BF)
    allowed = mask_ref[...] > 0.5
    parts = []
    for h in range(HEADS // 2):
        qh = packed[:, h * HD : (h + 1) * HD]
        kh = packed[:, HALF + h * HD : HALF + (h + 1) * HD]
        vh = packed[:, 2 * HALF + h * HD : 2 * HALF + (h + 1) * HD]
        scores = lax.dot_general(qh, kh, (((1,), (1,)), ((), ())), preferred_element_type=F32)
        scores = jnp.where(allowed, scores * (1.0 / math.sqrt(HD)), NEG)
        top = jnp.max(scores, axis=1, keepdims=True)
        probs = jnp.exp(scores - top)
        whole = jnp.sum(probs, axis=1, keepdims=True)
        parts.append(jnp.dot(probs.astype(BF), vh, preferred_element_type=F32) / whole)
    mixed = jnp.concatenate(parts, axis=1)
    for i in range(NF):
        rets[i] = mixed[i * GROUP : (i + 1) * GROUP].astype(BF)

    def send_ret(i, _):
        to = (f + i) % NF
        remote(rets.at[to], retgot.at[f], ret_s, ret_r, to, s).start()
        return 0

    lax.fori_loop(1, NF, send_ret, 0)
    retgot[f] = rets[f]

    for copy in (wp_y, wp_c, wt_y, wt_c, wp_more, wt_more):
        copy.wait_send()
    for m, buf in ((0, wp), (1, wt)):
        for k in range(4):
            for i in range(NP):
                ring(m, buf, k, i).wait_send()
            for n in range(NC):
                die(m, buf, k, n).wait_send()
            swap(m, buf, k, 1).wait_send()
    total(pack, NS - 1, qkv_s).wait_send()
    total(att, NS - 1, att_s).wait_send()
    for i in range(2):
        n = 16 if i == 0 else 15
        remote(toks.at[pl.ds(0, n)], toks.at[pl.ds(0, n)], tok_s, tok_s, f, s).wait_send()
    total(rets, NF - 1, ret_s).wait_send()

    total(retgot, NF - 1, ret_r).wait_recv()
    for g in range(0, 16, 2):
        pair = [jnp.concatenate([retgot[i].astype(F32), retgot[16 + i].astype(F32)], axis=1) for i in (g, g + 1)]
        out_ref[pl.ds(g * GROUP, 2 * GROUP), :] = jnp.concatenate(pair, axis=0)
    last = pltpu.make_async_copy(out_ref, temporal_out, local.at[7])
    last.start()
    keep.wait()
    last.wait()


def shards(q, k, v, lat, wp, bias, gate, shift, scale, wt, clips):
    flat2 = lambda a: a.reshape(ROWS, D)
    vmem = pl.BlockSpec(memory_space=pltpu.VMEM)
    hbm = pl.BlockSpec(memory_space=pl.ANY)
    hidden, temporal = pl.pallas_call(
        kernel,
        out_shape=(
            jax.ShapeDtypeStruct((ROWS, D), F32),
            jax.ShapeDtypeStruct((ROWS, D), F32),
        ),
        in_specs=[pl.BlockSpec(memory_space=pltpu.SMEM)] + [hbm] * 6 + [vmem] * 4,
        out_specs=(hbm, hbm),
        scratch_shapes=[
            pltpu.VMEM((ROWS, D), BF),
            pltpu.VMEM((ROWS, D), BF),
            pltpu.VMEM((ROWS, D), BF),
            pltpu.VMEM((ROWS, D), BF),
            pltpu.VMEM((SHARD, D), BF),
            pltpu.VMEM((SHARD, 3 * D), BF),
            pltpu.VMEM((ROWS, D), F32),
            pltpu.VMEM((ROWS, D), F32),
            pltpu.SemaphoreType.DMA((8,)),
            pltpu.VMEM((NS, ROWS, 256), BF),
            pltpu.VMEM((NS, ROWS, 256), BF),
            pltpu.VMEM((NS, ROWS, 128), BF),
            pltpu.VMEM((NS, ROWS, 128), BF),
            pltpu.VMEM((4, SHARD, D), BF),
            pltpu.VMEM((4, SHARD, WIDE), BF),
            pltpu.VMEM((NZ, QUAD, D), BF),
            pltpu.VMEM((NZ, QUAD, WIDE), BF),
            pltpu.VMEM((ROWS // GROUP, GROUP, D), BF),
            pltpu.VMEM((NF, GROUP, D), BF),
            pltpu.VMEM((NF, GROUP, HALF), BF),
            pltpu.VMEM((NF, GROUP, HALF), BF),
            pltpu.VMEM((ROWS, D), F32),
            pltpu.VMEM((TOK, TOK), F32),
            pltpu.VMEM((SHARD, WIDE), BF),
        ]
        + [pltpu.SemaphoreType.DMA] * 8
        + [
            pltpu.SemaphoreType.DMA((6,)),
            pltpu.SemaphoreType.DMA((6,)),
            pltpu.SemaphoreType.DMA((8 * NP,)),
            pltpu.SemaphoreType.DMA((8 * NP,)),
            pltpu.SemaphoreType.DMA((8 * NC,)),
            pltpu.SemaphoreType.DMA((8 * NC,)),
            pltpu.SemaphoreType.DMA((8,)),
            pltpu.SemaphoreType.DMA((8,)),
        ],
        compiler_params=pltpu.CompilerParams(
            collective_id=0, has_side_effects=True, vmem_limit_bytes=56 * 1024 * 1024
        ),
        name="stdit",
    )(clips, flat2(q), flat2(k), flat2(v), flat2(lat), wp, wt, bias, gate, shift, scale)
    return hidden.reshape(1, ROWS, D), temporal.reshape(1, ROWS, D)


def solution(mesh):
    both = P("frame", "space", None)
    return jax.shard_map(
        shards,
        mesh=mesh,
        in_specs=(both, both, both, both, P("frame", None), P(), P(), P(), P(), P("frame", None), P()),
        out_specs=(both, both),
        check_vma=False,
    )
```

```python
import math

import jax
import jax.numpy as jnp
from jax import lax
from jax.experimental import pallas as pl
from jax.experimental.pallas import tpu as pltpu
from jax.sharding import PartitionSpec as P

MESH = pl.DeviceIdType.MESH
BF = jnp.bfloat16
F32 = jnp.float32

HEADS = 16
HD = 72
D = HEADS * HD
NS = 16
NF = 32
ROWS = 64
NZ = 8
SHARD = 36
QUAD = 4 * SHARD
HALF = D // 2
WT = 3 * HALF
GROUP = 4
TOK = NF * GROUP
NEG = -1e30
LOG2E = 1.4426950408889634
WIDE = 14 * 128
RINGED = ((512, 640), (896, 896))
SWAPPED = ((640, 512), (896, 896))
PIECES = (((0, 256), (256, 384)), ((0, 512), (512, 384)))
NC = 2
NP = 2

ORDER = tuple((j % 2) * 8 + j // 2 for j in range(HEADS))


def remote(src, dst, send, recv, f, s):
    return pltpu.make_async_remote_copy(
        src_ref=src, dst_ref=dst, send_sem=send, recv_sem=recv, device_id=(f, s), device_id_type=MESH
    )


def kernel(
    clip_ref, q_in, k_in, v_in, lat_in, wp_in, wt_in, bias_ref, gate_ref, shift_ref, scale_ref,
    hidden_out, temporal_out,
    q_ref, k_ref, v_ref, lat_ref, wp_ref, wt_ref, hidden_ref, out_ref, local,
    pack, got, att, attgot, wpq, wtq, wp, wt, toks, tokgot, rets, retgot, flat, mask_ref, wto,
    qkv_s, qkv_r, att_s, att_r, tok_s, tok_r, ret_s, ret_r,
    pre_s, pre_r, ring_s, ring_r, die_s, die_r, swap_s, swap_r,
):
    f = lax.axis_index("frame")
    s = lax.axis_index("space")
    row = f // 16
    z = (f // 2) % NZ
    c = f % 2
    group = f % 16
    yhi = s % 4
    step = 1 - 2 * c
    fz = row * 16 + ((z + step + NZ) % NZ) * 2 + c
    sib = row * 16 + z * 2 + (1 - c)
    other = (1 - row) * 16 + z * 2 + c
    sb = (s - yhi) + (yhi + 2 * row - 1 + 4) % 4
    me_q = row * 2 + c
    other_q = (1 - row) * 2 + c
    x = s // 4
    part = (x % 2, x // 2)
    beside = (s + 4 * (1 - 2 * (x % 2)), (3 - x) * 4 + yhi)

    loads = [
        pltpu.make_async_copy(src, dst, local.at[i])
        for i, (src, dst) in enumerate(
            ((wp_in, wp_ref), (wt_in, wt_ref), (k_in, k_ref), (q_in, q_ref), (v_in, v_ref), (lat_in, lat_ref))
        )
    ]
    for load in loads:
        load.start()

    barrier = pltpu.get_barrier_semaphore()

    def hail_space(i, _):
        pl.semaphore_signal(barrier, inc=1, device_id=(f, (s + i) % NS), device_id_type=MESH)
        return 0

    def hail_frame(i, _):
        pl.semaphore_signal(barrier, inc=1, device_id=((f + i) % NF, s), device_id_type=MESH)
        return 0

    lax.fori_loop(1, NS, hail_space, 0)
    lax.fori_loop(1, NF, hail_frame, 0)
    pl.semaphore_signal(barrier, inc=1, device_id=(other, sb), device_id_type=MESH)

    for load in loads:
        load.wait()
    for h in range(HEADS):
        cut = pl.ds(h * HD, HD)
        kk, qq, vv = k_ref[:, cut], q_ref[:, cut], v_ref[:, cut]
        pack[h, :, 0:128] = jnp.concatenate([kk, qq[:, :56]], axis=1)
        pack[h, :, 128:256] = jnp.concatenate([vv, qq[:, 56:], jnp.zeros((ROWS, 40), BF)], axis=1)
    wpq[me_q] = wp_ref[...]
    for r in range(2):

        @pl.when(row == r)
        def _():
            mine = [wt_ref[:, pl.ds(t * D + r * HALF, HALF)] for t in range(3)]
            rest = [wt_ref[:, pl.ds(t * D + (1 - r) * HALF, HALF)] for t in range(3)]
            pad = [jnp.zeros((SHARD, WIDE - WT), BF)]
            wtq[me_q] = jnp.concatenate(mine + pad, axis=1)
            wto[...] = jnp.concatenate(rest + pad, axis=1)

    pl.semaphore_wait(barrier, NS - 1 + NF - 1 + 1)

    wp_y = remote(wp_ref, wpq.at[me_q], pre_s.at[0], pre_r.at[0], other, sb)
    wp_c = remote(wp_ref, wpq.at[me_q], pre_s.at[1], pre_r.at[1], sib, s)
    wp_y.start()
    wp_c.start()
    wt_y = remote(wto, wtq.at[me_q], pre_s.at[2], pre_r.at[2], other, s)
    wt_c = remote(wtq.at[me_q], wtq.at[me_q], pre_s.at[3], pre_r.at[3], sib, s)
    wt_y.start()
    wt_c.start()

    def send_qkv(i, _):
        to = (s + i) % NS
        remote(pack.at[to], got.at[s], qkv_s, qkv_r, f, to).start()
        return 0

    lax.fori_loop(1, NS, send_qkv, 0)
    got[s] = pack[s]

    def piece(m, buf, block, k, first, rows, kind, own, skip=0, width=None):
        apart, whole = kind[m]
        which = part[m] if own else 1 - part[m]
        cut = pl.ds(pl.multiple_of(which * apart + skip, 128), width or whole)
        block = (block + 2 * NZ) % NZ
        if k < 3:
            return buf.at[block, :, cut]
        return buf.at[block, pl.ds(pl.multiple_of(first, 16), rows), cut]

    def ring(m, buf, k, i):
        src = piece(m, buf, z - step * k, k, c * 64, 80, RINGED, True, *PIECES[m][i])
        at = (m * 4 + k) * NP + i
        return remote(src, src, ring_s.at[at], ring_r.at[at], fz, s)

    def ring_arrived(m, buf, k, i):
        dst = piece(m, buf, z - step * (k + 1), k, c * 64, 80, RINGED, True, *PIECES[m][i])
        at = (m * 4 + k) * NP + i
        return remote(dst, dst, ring_s.at[at], ring_r.at[at], fz, s)

    def die(m, buf, k, n):
        src = piece(m, buf, z - step * (k + 1), k, c * 80, 64, *((RINGED, True) if n == 0 else (SWAPPED, False)))
        at = (m * 4 + k) * NC + n
        return remote(src, src, die_s.at[at], die_r.at[at], sib, s)

    def die_arrived(m, buf, k, n):
        dst = piece(m, buf, z + step * (k + 1), k, (1 - c) * 80, 64, *((RINGED, True) if n == 0 else (SWAPPED, False)))
        at = (m * 4 + k) * NC + n
        return remote(dst, dst, die_s.at[at], die_r.at[at], sib, s)

    def swap(m, buf, k, n):
        ref = piece(m, buf, z - step * (k + 1), k, c * 64, 80, SWAPPED, n == 1)
        return remote(ref, ref, swap_s.at[m * 4 + k], swap_r.at[m * 4 + k], f, beside[m])

    def relay(m, buf, k):
        for i in range(NP):
            ring_arrived(m, buf, k, i).wait_recv()
            if k < 3:
                ring(m, buf, k + 1, i).start()
        swap(m, buf, k, 1).start()
        die(m, buf, k, 0).start()

    def swapped(m, buf, k):
        swap(m, buf, k, 2).wait_recv()
        die(m, buf, k, 1).start()

    def begin(m, quads, buf, over_y, over_c):
        over_y.wait_recv()
        more = remote(quads.at[other_q], quads.at[other_q], pre_s.at[4 + m], pre_r.at[4 + m], sib, s)
        more.start()
        over_c.wait_recv()
        more.wait_recv()
        buf[z] = jnp.concatenate([quads[i].astype(F32) for i in range(4)], axis=0).astype(BF)
        for i in range(NP):
            ring(m, buf, 0, i).start()
        return more

    wp_more = begin(0, wpq, wp, wp_y, wp_c)

    ri = lax.broadcasted_iota(jnp.int32, (TOK, TOK), 0)
    ci = lax.broadcasted_iota(jnp.int32, (TOK, TOK), 1)
    clip_r = jnp.zeros((TOK, TOK), jnp.int32)
    clip_c = jnp.zeros((TOK, TOK), jnp.int32)
    end = jnp.int32(0)
    for i in range(clip_ref.shape[0]):
        end = end + clip_ref[i]
        clip_r = clip_r + jnp.where(ri >= GROUP * end, 1, 0)
        clip_c = clip_c + jnp.where(ci >= GROUP * end, 1, 0)
    same = (clip_r == clip_c) & ((ri % GROUP) == (ci % GROUP))
    mask_ref[...] = jnp.where(same, 1.0, 0.0)

    wt_more = begin(1, wtq, wt, wt_y, wt_c)
    relay(0, wp, 0)
    relay(1, wt, 0)
    relay(0, wp, 1)

    def total(buf, n, recv):
        return remote(buf.at[pl.ds(0, n)], buf.at[pl.ds(0, n)], recv, recv, f, s)

    total(got, NS - 1, qkv_r).wait_recv()

    lane = lax.broadcasted_iota(jnp.int32, (NS * ROWS, 128), 1)
    left = got[:, :, 0:128].reshape(NS * ROWS, 128)
    right = got[:, :, 128:256].reshape(NS * ROWS, 128)
    values = jnp.where(lane < HD, right.astype(F32), jnp.where(lane == HD, 1.0, 0.0)).astype(BF)
    qblock = 256
    factor = LOG2E / math.sqrt(HD)
    qlane = lax.broadcasted_iota(jnp.int32, (qblock, 128), 1)

    for i in range(NS * ROWS // qblock):
        lo = left[i * qblock : (i + 1) * qblock].astype(F32)
        hi = right[i * qblock : (i + 1) * qblock].astype(F32)
        query = jnp.where(
            qlane < 56, pltpu.roll(lo, 56, 1), jnp.where(qlane < HD, pltpu.roll(hi, 112, 1), 0.0)
        ).astype(BF)
        scores = lax.dot_general(query, left, (((1,), (1,)), ((), ())), preferred_element_type=F32)
        top = jnp.max(scores, axis=1, keepdims=True)
        probs = jnp.exp2((scores - top) * factor).astype(BF)
        mixed = jnp.dot(probs, values, preferred_element_type=F32)
        mixed = (mixed / mixed[:, HD : HD + 1]).astype(BF)
        each = qblock // ROWS
        att[pl.ds(i * each, each)] = mixed.reshape(each, ROWS, 128)
        for j in range(each):
            to = i * each + j

            @pl.when(s != to)
            def _():
                remote(att.at[to], attgot.at[s], att_s, att_r, f, to).start()

        if i == 1:
            relay(1, wt, 1)
        if i == 3:
            relay(0, wp, 2)
    attgot[s] = att[s]

    swapped(0, wp, 0)
    swapped(0, wp, 1)
    relay(0, wp, 3)
    relay(1, wt, 2)
    swapped(0, wp, 2)
    swapped(0, wp, 3)

    total(attgot, NS - 1, att_r).wait_recv()
    rows = jnp.concatenate([attgot[h, :, 0:HD] for h in ORDER], axis=1)
    for k in range(4):
        for n in range(NC):
            die_arrived(0, wp, k, n).wait_recv()
    projected = jnp.dot(rows, wp[...].reshape(D, D), preferred_element_type=F32)
    relay(1, wt, 3)
    hidden = lat_ref[...].astype(F32) + gate_ref[...] * (projected + bias_ref[...])
    hidden_ref[...] = hidden
    keep = pltpu.make_async_copy(hidden_ref, hidden_out, local.at[6])
    keep.start()
    mean = jnp.mean(hidden, axis=1, keepdims=True)
    centred = hidden - mean
    variance = jnp.mean(centred * centred, axis=1, keepdims=True)
    flat[...] = centred * lax.rsqrt(variance + 1e-06) * (1.0 + scale_ref[...]) + shift_ref[...]
    normed = jnp.concatenate([flat[:, pl.ds(h * HD, HD)] for h in ORDER], axis=1)
    for g in range(ROWS // GROUP):
        toks[g] = normed[g * GROUP : (g + 1) * GROUP].astype(BF)

    def send_tok(i, _):
        to = (f + i) % NF
        remote(toks.at[to % 16], tokgot.at[f], tok_s, tok_r, to, s).start()
        return 0

    lax.fori_loop(1, NF, send_tok, 0)
    tokgot[f] = toks[group]

    swapped(1, wt, 0)
    swapped(1, wt, 1)
    swapped(1, wt, 2)
    swapped(1, wt, 3)
    total(tokgot, NF - 1, tok_r).wait_recv()
    tokens = jnp.concatenate([tokgot[i].astype(F32) for i in range(NF)], axis=0).astype(BF)
    for k in range(4):
        for n in range(NC):
            die_arrived(1, wt, k, n).wait_recv()
    packed = jnp.dot(tokens, wt[...].reshape(D, WIDE), preferred_element_type=F32).astype(BF)
    allow = mask_ref[...]
    for half in range(2):
        rows_of = slice(half * TOK // 2, (half + 1) * TOK // 2)
        parts = []
        for h in range(HEADS // 2):
            qh = packed[rows_of, h * HD : (h + 1) * HD]
            kh = packed[:, HALF + h * HD : HALF + (h + 1) * HD]
            vh = packed[:, 2 * HALF + h * HD : 2 * HALF + (h + 1) * HD]
            scores = lax.dot_general(qh, kh, (((1,), (1,)), ((), ())), preferred_element_type=F32)
            scores = jnp.where(allow[rows_of] > 0.5, scores * (1.0 / math.sqrt(HD)), NEG)
            top = jnp.max(scores, axis=1, keepdims=True)
            probs = jnp.exp(scores - top)
            whole = jnp.sum(probs, axis=1, keepdims=True)
            parts.append(jnp.dot(probs.astype(BF), vh, preferred_element_type=F32) / whole)
        mixed = jnp.concatenate(parts, axis=1)
        for i in range(NF // 2):
            rets[half * NF // 2 + i] = mixed[i * GROUP : (i + 1) * GROUP].astype(BF)

        def send_ret(i, _):
            to = half * (NF // 2) + (f + i) % (NF // 2)

            @pl.when(to != f)
            def _():
                remote(rets.at[to], retgot.at[f], ret_s, ret_r, to, s).start()

            return 0

        lax.fori_loop(0, NF // 2, send_ret, 0)
    retgot[f] = rets[f]

    for copy in (wp_y, wp_c, wt_y, wt_c, wp_more, wt_more):
        copy.wait_send()
    for m, buf in ((0, wp), (1, wt)):
        for k in range(4):
            for i in range(NP):
                ring(m, buf, k, i).wait_send()
            for n in range(NC):
                die(m, buf, k, n).wait_send()
            swap(m, buf, k, 1).wait_send()
    total(pack, NS - 1, qkv_s).wait_send()
    total(att, NS - 1, att_s).wait_send()
    for i in range(2):
        n = 16 if i == 0 else 15
        remote(toks.at[pl.ds(0, n)], toks.at[pl.ds(0, n)], tok_s, tok_s, f, s).wait_send()
    total(rets, NF - 1, ret_s).wait_send()

    total(retgot, NF - 1, ret_r).wait_recv()
    for g in range(0, 16, 2):
        pair = [jnp.concatenate([retgot[i].astype(F32), retgot[16 + i].astype(F32)], axis=1) for i in (g, g + 1)]
        out_ref[pl.ds(g * GROUP, 2 * GROUP), :] = jnp.concatenate(pair, axis=0)
    last = pltpu.make_async_copy(out_ref, temporal_out, local.at[7])
    last.start()
    keep.wait()
    last.wait()


def shards(q, k, v, lat, wp, bias, gate, shift, scale, wt, clips):
    flat2 = lambda a: a.reshape(ROWS, D)
    vmem = pl.BlockSpec(memory_space=pltpu.VMEM)
    hbm = pl.BlockSpec(memory_space=pl.ANY)
    hidden, temporal = pl.pallas_call(
        kernel,
        out_shape=(
            jax.ShapeDtypeStruct((ROWS, D), F32),
            jax.ShapeDtypeStruct((ROWS, D), F32),
        ),
        in_specs=[pl.BlockSpec(memory_space=pltpu.SMEM)] + [hbm] * 6 + [vmem] * 4,
        out_specs=(hbm, hbm),
        scratch_shapes=[
            pltpu.VMEM((ROWS, D), BF),
            pltpu.VMEM((ROWS, D), BF),
            pltpu.VMEM((ROWS, D), BF),
            pltpu.VMEM((ROWS, D), BF),
            pltpu.VMEM((SHARD, D), BF),
            pltpu.VMEM((SHARD, 3 * D), BF),
            pltpu.VMEM((ROWS, D), F32),
            pltpu.VMEM((ROWS, D), F32),
            pltpu.SemaphoreType.DMA((8,)),
            pltpu.VMEM((NS, ROWS, 256), BF),
            pltpu.VMEM((NS, ROWS, 256), BF),
            pltpu.VMEM((NS, ROWS, 128), BF),
            pltpu.VMEM((NS, ROWS, 128), BF),
            pltpu.VMEM((4, SHARD, D), BF),
            pltpu.VMEM((4, SHARD, WIDE), BF),
            pltpu.VMEM((NZ, QUAD, D), BF),
            pltpu.VMEM((NZ, QUAD, WIDE), BF),
            pltpu.VMEM((ROWS // GROUP, GROUP, D), BF),
            pltpu.VMEM((NF, GROUP, D), BF),
            pltpu.VMEM((NF, GROUP, HALF), BF),
            pltpu.VMEM((NF, GROUP, HALF), BF),
            pltpu.VMEM((ROWS, D), F32),
            pltpu.VMEM((TOK, TOK), F32),
            pltpu.VMEM((SHARD, WIDE), BF),
        ]
        + [pltpu.SemaphoreType.DMA] * 8
        + [
            pltpu.SemaphoreType.DMA((6,)),
            pltpu.SemaphoreType.DMA((6,)),
            pltpu.SemaphoreType.DMA((8 * NP,)),
            pltpu.SemaphoreType.DMA((8 * NP,)),
            pltpu.SemaphoreType.DMA((8 * NC,)),
            pltpu.SemaphoreType.DMA((8 * NC,)),
            pltpu.SemaphoreType.DMA((8,)),
            pltpu.SemaphoreType.DMA((8,)),
        ],
        compiler_params=pltpu.CompilerParams(
            collective_id=0, has_side_effects=True, vmem_limit_bytes=56 * 1024 * 1024
        ),
        name="stdit",
    )(clips, flat2(q), flat2(k), flat2(v), flat2(lat), wp, wt, bias, gate, shift, scale)
    return hidden.reshape(1, ROWS, D), temporal.reshape(1, ROWS, D)


def solution(mesh):
    both = P("frame", "space", None)
    return jax.shard_map(
        shards,
        mesh=mesh,
        in_specs=(both, both, both, both, P("frame", None), P(), P(), P(), P(), P("frame", None), P()),
        out_specs=(both, both),
        check_vma=False,
    )
```
